32 devices in a mesh: scene: 2 (over y), tile: 4 (over z), half: 2 (over x), band: 2 (over core).
Axes of the slice: x: 2, y: 2, z: 4, core: 2. Of those that a mesh axis runs over, the one named last changes fastest.
Arguments:
- optical: bfloat16 [16, 2, 512, 512], P(('scene', 'tile'), 'band', 'half'), parts along dimension 0, may hold values from -64 to 64
- sar: bfloat16 [2, 8192, 512], P('band', ('scene', 'tile', 'half')), parts along dimension 1, may hold values from -64 to 64
- destination: int32 [128], P('scene'), parts along dimension 0, may hold values from 0 to 63, as said below
- peaks: int32 [16, 2, 8], P(('scene', 'tile', 'band')), parts along dimension 0, may hold values from 0 to 511
Outputs:
- surface: float32 [16, 512, 512], P(('scene', 'tile', 'band'), 'half'), parts along dimension 0
- peak_values: float32 [16, 8], P(('scene', 'tile', 'band')), parts along dimension 0
The draws below stay inside these ranges and needn't reach their ends.
There are 2 independent parts, one for each index of `scene`. The reference program is written for one: setup_inputs(seed, part) draws one part's arguments, and reference() takes and returns one part's arrays. A program takes and returns all parts, laid end to end along the dimension named above; each array names one. Nothing has to cross between parts.
Inputs may be any that keep to these rules, and one draw needn't show every extreme that they name: destination holds every block position 0 to 63 once; the 8 blocks that start at each multiple of 8 are sent one into each run of 8 positions that starts at a multiple of 8.
All inputs are finite; a program needn't handle non-finite values.
Results may differ from the reference program's by a relative error of at most 0.014.
Values may be sent and summed in bfloat16 or wider, within the bound.
A program may use at most 64 MiB of HBM per device.

```python
import math
import jax
import jax.numpy as jnp
from jax import lax

PATCH_SIZE = 512
BAND_COUNT = 2
PATCH_DEV = 2
PEAK_COUNT = 8
PATCHES = 8
GROUP_DEVICES = 8
BLOCK_LINES = 64
BLOCKS = 64
SLANT_LINES = 4096
N_TILE = 4
N_HALF = 2


def one_order(subkey):
    return jax.random.permutation(subkey, GROUP_DEVICES).astype(jnp.int32)


def draw_destination(key, part):
    subkeys = jax.random.split(jax.random.fold_in(key, 7), 2)
    sending = jax.vmap(one_order)(jax.random.split(subkeys[0], GROUP_DEVICES))
    slotting = jax.vmap(one_order)(jax.random.split(subkeys[1], GROUP_DEVICES))
    senders = jnp.arange(GROUP_DEVICES, dtype=jnp.int32)[:, None]
    slot_index = slotting[sending, senders]
    return (sending * GROUP_DEVICES + slot_index).reshape(BLOCKS).astype(jnp.int32)


def draw_optical(key, part):
    full_shape = (PATCHES, BAND_COUNT, PATCH_SIZE, PATCH_SIZE)
    line_frac = jnp.arange(PATCH_SIZE, dtype=jnp.float32)[:, None] / (PATCH_SIZE - 1)
    subkeys = jax.random.split(jax.random.fold_in(key, 3), 1)
    noise_draw = jnp.clip(jax.random.normal(subkeys[0], full_shape, jnp.float32), -5.0, 5.0)
    values = noise_draw * jnp.exp(math.log(3.0) * line_frac - 0.5 * math.log(3.0))
    return values.astype(jnp.bfloat16)


def draw_sar(key, part):
    full_shape = (BAND_COUNT, SLANT_LINES, PATCH_SIZE)
    line_frac = jnp.arange(SLANT_LINES, dtype=jnp.float32)[:, None] / (SLANT_LINES - 1)
    subkeys = jax.random.split(jax.random.fold_in(key, 5), 1)
    noise_draw = jnp.clip(jax.random.normal(subkeys[0], full_shape, jnp.float32), -5.0, 5.0)
    values = noise_draw * jnp.exp(math.log(3.0) * line_frac - 0.5 * math.log(3.0))
    return values.astype(jnp.bfloat16)


def place_ends(entries, own_key, low, high):
    index_at = [jax.random.randint(jax.random.fold_in(own_key, axis), (), 0, length) for axis, length in enumerate(entries.shape)]
    longest = entries.shape.index(max(entries.shape))
    neighbour = index_at[:longest] + [(index_at[longest] + 1) % entries.shape[longest]] + index_at[longest + 1:]
    return entries.at[tuple(index_at)].set(low).at[tuple(neighbour)].set(high)


def setup_inputs(seed: int = 0, part: int = 0) -> dict:
    key_list = jax.random.split(jax.random.key(seed), 5)
    part_splits = jax.random.split(jax.random.fold_in(key_list[4], part), 5)
    optical = draw_optical(jax.random.fold_in(jax.random.fold_in(key_list[4], part), 71), part)
    sar = draw_sar(jax.random.fold_in(jax.random.fold_in(key_list[4], part), 71), part)
    destination = draw_destination(jax.random.fold_in(jax.random.fold_in(key_list[4], part), 71), part)
    peaks = place_ends(jax.random.randint(part_splits[3], (PATCHES, 2, PEAK_COUNT), 0, PATCH_SIZE), jax.random.fold_in(part_splits[3], 1), 0, PATCH_SIZE - 1).astype(jnp.int32)
    return dict(optical=optical, sar=sar, destination=destination, peaks=peaks)


EPSILON = 1e-06

def column_pair(samples):
    spectrum = jnp.fft.fft(samples.astype(jnp.float32), axis=-1)
    return (jnp.real(spectrum).astype(jnp.bfloat16), jnp.imag(spectrum).astype(jnp.bfloat16))

def line_spectrum(samples):
    real_part, imag_part = column_pair(samples)
    joined = real_part.astype(jnp.float32) + 1j * imag_part.astype(jnp.float32)
    spectrum = jnp.fft.fft(joined, axis=-2)
    return spectrum.at[..., 0, 0].set(0.0)

def band_energy(samples):
    values = samples.astype(jnp.float32)
    total_sums = lax.optimization_barrier(jnp.sum(values, axis=(2, 3)))
    squares = lax.optimization_barrier(jnp.sum(values * values, axis=(2, 3)))
    pixel_count = PATCH_SIZE * PATCH_SIZE
    centered = squares - total_sums * total_sums / pixel_count
    return lax.optimization_barrier(jnp.sum(centered, axis=1)) / (BAND_COUNT * pixel_count)

def reference(optical, sar, destination, peaks):
    blocks = sar.reshape(BAND_COUNT, BLOCKS, BLOCK_LINES, PATCH_SIZE)
    placed = jnp.zeros_like(blocks).at[:, destination].set(blocks)
    sar_map = placed.reshape(BAND_COUNT, N_TILE, N_HALF, PATCH_DEV, PATCH_SIZE // N_HALF, PATCH_SIZE)
    sar_map = jnp.transpose(sar_map, (1, 3, 0, 2, 4, 5)).reshape(PATCHES, BAND_COUNT, PATCH_SIZE, PATCH_SIZE)
    opt_spec = line_spectrum(optical)
    sar_spec = line_spectrum(sar_map)
    opt_energy = band_energy(optical)
    sar_energy = band_energy(sar_map)
    cross_sum = lax.optimization_barrier(jnp.sum(jnp.conj(opt_spec) * sar_spec, axis=1))
    correlation = jnp.real(jnp.fft.ifft2(cross_sum, axes=(-2, -1)))
    pixel_count = PATCH_SIZE * PATCH_SIZE
    norm_scale = lax.rsqrt(BAND_COUNT * pixel_count * (opt_energy + EPSILON) * (sar_energy + EPSILON))
    surface = (correlation * norm_scale[:, None, None]).astype(jnp.float32)
    flattened = surface.reshape(PATCHES, pixel_count)
    spots = (peaks[:, 0, :] * PATCH_SIZE + peaks[:, 1, :]).astype(jnp.int32)
    peak_values = jnp.take_along_axis(flattened, spots, axis=1)
    return (surface, peak_values)
```

```python
import functools
import math

import jax
import jax.numpy as jnp
import numpy as np
from jax import lax
from jax.experimental import pallas as pl
from jax.experimental.pallas import tpu as pltpu
from jax.sharding import PartitionSpec as P

MESH = pl.DeviceIdType.MESH

precise = lax.Precision.HIGHEST
EPSILON = 1e-06


def fourier_tables(extent):
    places = jnp.arange(extent, dtype=jnp.int32)
    phases = places[:, None] * places[None, :] % extent
    angles = phases.astype(jnp.float32) * (2.0 * math.pi / extent)
    return (jnp.cos(angles), jnp.sin(angles))


def fourier_pair(table):
    upper = table.astype(jnp.bfloat16)
    lower = (table - upper.astype(jnp.float32)).astype(jnp.bfloat16)
    return (upper, lower)


def column_spectrum(samples, table_upper, table_lower):
    extent = samples.shape[-1]
    values = samples.reshape(-1, extent)
    spectrum = jnp.dot(values, table_upper, preferred_element_type=jnp.float32) + jnp.dot(
        values, table_lower, preferred_element_type=jnp.float32
    )
    return spectrum.astype(jnp.bfloat16).reshape(samples.shape[:-1] + (2 * extent,))


def row_spectrum(columns, table_upper, table_lower):
    line_count = columns.shape[-3]
    stacked = jnp.concatenate([columns[..., 0, :], columns[..., 1, :]], axis=-2)
    result = jnp.einsum("kr,...rc->...kc", table_upper, stacked, preferred_element_type=jnp.float32)
    result = result + jnp.einsum(
        "kr,...rc->...kc", table_lower, stacked, preferred_element_type=jnp.float32
    )
    return (result[..., :line_count, :], result[..., line_count:, :])


def relay_blocks(parcel):
    layout = parcel.shape
    merged = parcel.reshape(layout[:1] + (layout[1] * layout[2],) + layout[3:])
    arrived = lax.all_to_all(merged, ("tile", "half"), split_axis=1, concat_axis=1, tiled=True)
    return arrived.reshape(layout)


def generic(optical, sar, destination, peaks):
    tile_count = lax.axis_size("tile")
    half_count = lax.axis_size("half")
    band_count = lax.axis_size("band")
    group_size = tile_count * half_count
    patch_dev, local_bands, quarter, extent = optical.shape
    col_width = extent // half_count
    block_lines = sar.shape[1] // group_size
    band_total = local_bands * band_count
    pixel_count = extent * extent
    patch_total = patch_dev * tile_count
    kept_patches = patch_dev // band_count
    cosine_table, sine_table = fourier_tables(extent)
    col_upper, col_lower = fourier_pair(jnp.concatenate([cosine_table, -sine_table], axis=1))
    row_full = jnp.concatenate(
        [
            jnp.concatenate([cosine_table, sine_table], axis=1),
            jnp.concatenate([-sine_table, cosine_table], axis=1),
        ],
        axis=0,
    )
    row_upper, row_lower = fourier_pair(row_full)
    tile_at = lax.axis_index("tile")
    half_at = lax.axis_index("half")
    band_at = lax.axis_index("band")
    device_at = lax.axis_index(("tile", "half"))
    own_blocks = lax.dynamic_slice_in_dim(destination, device_at * group_size, group_size)
    send_order = jnp.argsort(own_blocks // group_size)
    inverse = (
        jnp.zeros_like(destination)
        .at[destination]
        .set(jnp.arange(destination.shape[0], dtype=jnp.int32))
    )
    opt_values = optical.astype(jnp.float32)
    opt_sums = jnp.sum(opt_values, axis=(2, 3))
    opt_squares = jnp.sum(opt_values * opt_values, axis=(2, 3))
    sar_values = sar.astype(jnp.float32).reshape(local_bands, group_size, block_lines * extent)
    sar_sums = jnp.sum(sar_values, axis=2)
    sar_squares = jnp.sum(sar_values * sar_values, axis=2)
    map_device = own_blocks // group_size
    map_patch = (
        map_device // half_count * patch_dev + own_blocks % group_size * block_lines // quarter
    )
    member = (map_patch[:, None] == jnp.arange(patch_total, dtype=jnp.int32)[None, :]).astype(
        jnp.float32
    )
    sar_stats = jnp.dot(
        jnp.stack([sar_sums, sar_squares]).reshape(2 * local_bands, group_size),
        member,
        precision=precise,
        preferred_element_type=jnp.float32,
    )
    statistics = jnp.zeros((2, 2, band_total, patch_total), jnp.float32)
    opt_part = jnp.transpose(jnp.stack([opt_sums, opt_squares]), (0, 2, 1))
    statistics = lax.dynamic_update_slice(
        statistics, opt_part[None], (0, 0, band_at * local_bands, tile_at * patch_dev)
    )
    statistics = lax.dynamic_update_slice(
        statistics,
        sar_stats.reshape(2, local_bands, patch_total)[None],
        (1, 0, band_at * local_bands, 0),
    )
    totals = lax.psum(statistics, ("tile", "half", "band"))
    centered = totals[:, 1] - totals[:, 0] * totals[:, 0] / pixel_count
    energy = jnp.sum(centered, axis=1) / (band_total * pixel_count)
    norm_scale = lax.rsqrt(band_total * pixel_count * (energy[0] + EPSILON) * (energy[1] + EPSILON))
    first_patch = tile_at * patch_dev + band_at * kept_patches
    norm_mine = lax.dynamic_slice_in_dim(norm_scale, first_patch, kept_patches)
    slant_spectra = column_spectrum(sar, col_upper, col_lower).reshape(
        local_bands, group_size, block_lines, 2, half_count, col_width
    )
    outgoing = jnp.take(slant_spectra, send_order, axis=1).reshape(
        local_bands, tile_count, half_count, block_lines, 2, half_count, col_width
    )
    outgoing = jnp.transpose(outgoing, (0, 1, 5, 2, 3, 4, 6))
    arrived = relay_blocks(outgoing).reshape(
        local_bands, group_size * half_count, block_lines, 2, col_width
    )
    sources = lax.dynamic_slice_in_dim(
        inverse, tile_at * half_count * group_size, half_count * group_size
    )
    slot_index = (
        sources // group_size * half_count
        + jnp.arange(half_count * group_size, dtype=jnp.int32) // group_size
    )
    placed = jnp.take(arrived, slot_index, axis=1).reshape(
        local_bands, half_count, patch_dev, quarter, 2, col_width
    )
    placed = jnp.transpose(placed, (2, 0, 1, 3, 4, 5)).reshape(
        patch_dev, local_bands, extent, 2, col_width
    )
    sar_real, sar_imag = row_spectrum(placed, row_upper, row_lower)
    spectra = column_spectrum(optical, col_upper, col_lower).reshape(
        patch_dev, local_bands, quarter, 2, half_count, col_width
    )
    real_part, imag_part = row_spectrum(
        jnp.squeeze(
            lax.all_to_all(spectra, "half", split_axis=4, concat_axis=2, tiled=True), axis=4
        ),
        row_upper,
        row_lower,
    )
    opt_real = real_part
    opt_imag = imag_part
    rows_at = jnp.arange(extent, dtype=jnp.int32)[:, None]
    cols_at = half_at * col_width + jnp.arange(col_width, dtype=jnp.int32)[None, :]
    keep_mask = jnp.where((rows_at == 0) & (cols_at == 0), 0.0, 1.0).astype(jnp.float32)
    opt_real = opt_real * keep_mask
    opt_imag = opt_imag * keep_mask
    sar_real = sar_real * keep_mask
    sar_imag = sar_imag * keep_mask
    cross_real = jnp.sum(opt_real * sar_real + opt_imag * sar_imag, axis=1)
    cross_imag = jnp.sum(opt_real * sar_imag - opt_imag * sar_real, axis=1)
    cross_term = jnp.stack([cross_real, cross_imag], axis=1)
    cross_sum = lax.psum_scatter(cross_term, "band", scatter_dimension=0, tiled=True)
    lag_real = (
        jnp.einsum("uk,pkc->puc", cosine_table, cross_sum[:, 0], precision=precise)
        - jnp.einsum("uk,pkc->puc", sine_table, cross_sum[:, 1], precision=precise)
    ) / extent
    lag_imag = (
        jnp.einsum("uk,pkc->puc", cosine_table, cross_sum[:, 1], precision=precise)
        + jnp.einsum("uk,pkc->puc", sine_table, cross_sum[:, 0], precision=precise)
    ) / extent
    lagged = jnp.stack([lag_real, lag_imag], axis=2).reshape(
        kept_patches, half_count, quarter, 2, col_width
    )
    pieces = lax.all_to_all(lagged, "half", split_axis=1, concat_axis=4, tiled=True)
    real_in = pieces[:, 0, :, 0, :]
    imag_in = pieces[:, 0, :, 1, :]
    correlation = (
        jnp.einsum("puc,cv->puv", real_in, cosine_table, precision=precise)
        - jnp.einsum("puc,cv->puv", imag_in, sine_table, precision=precise)
    ) / extent
    surface = correlation * norm_mine[:, None, None]
    local_rows = peaks[:, 0, :] - half_at * quarter
    row_hit = (
        local_rows[:, :, None] == jnp.arange(quarter, dtype=jnp.int32)[None, None, :]
    ).astype(jnp.float32)
    picked = jnp.einsum("pkr,prc->pkc", row_hit, surface, precision=precise)
    col_hit = (peaks[:, 1, :, None] == jnp.arange(extent, dtype=jnp.int32)[None, None, :]).astype(
        jnp.float32
    )
    local_values = jnp.sum(picked * col_hit, axis=2)
    peak_values = lax.psum(local_values, "half")
    return (surface, peak_values)


def half_tables(extent, half_count, chunk):
    width = extent // 2 // half_count
    places = np.arange(extent)
    phases = (places[:, None] * places[None, :]) % extent
    cosine = np.cos(phases * (2.0 * np.pi / extent))
    sine = np.sin(phases * (2.0 * np.pi / extent))
    forward, backward = [], []
    for half in range(half_count):
        span = slice(half * width, (half + 1) * width)
        real, imag = cosine[:, span].copy(), -sine[:, span]
        real_back, imag_back = 2.0 * cosine[span], -2.0 * sine[span]
        if half == 0:
            imag[:, 0] = cosine[:, extent // 2]
            real_back[0] = 1.0
            imag_back[0] = cosine[extent // 2]
        forward.append(np.concatenate([real, imag], axis=1))
        backward.append(np.concatenate([real_back, imag_back], axis=0))
    col_table = np.concatenate(forward, axis=1)
    lag_table = np.stack(backward)
    row_table = np.concatenate(
        [cosine.reshape(-1, chunk, extent), sine.reshape(-1, chunk, extent)], axis=1
    )
    return tuple(t.astype(jnp.bfloat16) for t in (col_table, row_table, lag_table))


def kernel(
    sizes,
    dest_ref,
    peaks_ref,
    sar_hbm,
    opt_hbm,
    col_hbm,
    row_hbm,
    lag_hbm,
    surface_ref,
    peak_ref,
    sar_v,
    opt_v,
    col_v,
    row_v,
    lag_v,
    sar_send,
    arrived,
    opt_send,
    opt_cols,
    sar_cols,
    sar_rows,
    cross_send,
    cross_recv,
    cross_own,
    cross_all,
    stat_send,
    stat_recv,
    last_send,
    last_recv,
    lags,
    lag_recv,
    load_sem,
    sar_ssem,
    sar_rsem,
    opt_ssem,
    opt_rsem,
    pair_ssem,
    pair_rsem,
):
    tiles, halves, bands, patch_dev, quarter, extent, lines, chunk, peak_count = sizes
    group = tiles * halves
    width = extent // 2 // halves
    chunks = extent // chunk
    per_half = chunks // halves
    tile, half, band = lax.axis_index("tile"), lax.axis_index("half"), lax.axis_index("band")
    me = tile * halves + half
    other_half = 1 - half
    other_band = 1 - band

    loads = [
        pltpu.make_async_copy(a, b, load_sem.at[i])
        for i, (a, b) in enumerate(
            [(sar_hbm, sar_v), (col_hbm, col_v), (opt_hbm, opt_v), (row_hbm, row_v), (lag_hbm, lag_v)]
        )
    ]
    for load in loads:
        load.start()

    barrier = pltpu.get_barrier_semaphore()
    for step in range(tiles):
        for shift in range(halves):
            if step or shift:
                pl.semaphore_signal(
                    barrier,
                    inc=1,
                    device_id={
                        "tile": lax.rem(tile + step, tiles),
                        "half": lax.rem(half + shift, halves),
                    },
                    device_id_type=MESH,
                )
    pl.semaphore_signal(barrier, inc=1, device_id={"band": other_band}, device_id_type=MESH)

    own_runs = [lax.div(dest_ref[me * group + j], group) for j in range(group)]

    def block_for(run):
        found = jnp.int32(0)
        for j in range(group):
            found = jnp.where(own_runs[j] == run, j, found)
        return found

    loads[0].wait()
    loads[1].wait()
    pl.semaphore_wait(barrier, group)

    def sar_copy(step, shift):
        to_half = lax.rem(half + shift, halves)
        return pltpu.make_async_remote_copy(
            src_ref=sar_send.at[step, to_half],
            dst_ref=arrived.at[me],
            send_sem=sar_ssem.at[step * halves + shift],
            recv_sem=sar_rsem.at[me],
            device_id={"tile": lax.rem(tile + step, tiles), "half": to_half},
            device_id_type=MESH,
        )

    copies = []
    order = sorted(range(tiles), key=lambda s: -min(s, tiles - s))
    for step in order:
        to_tile = lax.rem(tile + step, tiles)
        samples = jnp.concatenate(
            [sar_v[block_for(to_tile * halves + run)] for run in range(halves)], axis=0
        )
        spectra = jnp.dot(samples, col_v[...], preferred_element_type=jnp.float32)
        spectra = spectra.astype(jnp.bfloat16)
        for to_half in range(halves):
            piece = spectra[:, to_half * 2 * width : (to_half + 1) * 2 * width]
            sar_send[step, to_half] = piece.reshape(halves, lines, 2 * width)
        for shift in reversed(range(halves)):
            if step or shift:
                copy = sar_copy(step, shift)
                copy.start()
                copies.append(copy)
    arrived[me] = sar_send[0, half]

    opt_copies = []
    loads[2].wait()
    for turn, patch in enumerate((other_band, band)):
        spectra = jnp.dot(opt_v[patch], col_v[...], preferred_element_type=jnp.float32)
        spectra = spectra.astype(jnp.bfloat16)
        for to_half in range(halves):
            opt_send[turn, to_half] = spectra[:, to_half * 2 * width : (to_half + 1) * 2 * width]
        rows = pl.ds(pl.multiple_of(half * quarter, quarter), quarter)
        copy = pltpu.make_async_remote_copy(
            src_ref=opt_send.at[turn, other_half],
            dst_ref=opt_cols.at[turn, rows],
            send_sem=opt_ssem.at[turn],
            recv_sem=opt_rsem.at[turn],
            device_id={"half": other_half},
            device_id_type=MESH,
        )
        copy.start()
        opt_copies.append(copy)
        opt_cols[turn, rows, :] = opt_send[turn, half]

    slot_of = []
    for run in range(halves):
        places = []
        for source in range(group):
            place = jnp.int32(0)
            for j in range(group):
                spot = dest_ref[source * group + j]
                place = jnp.where(
                    lax.div(spot, group) == tile * halves + run, lax.rem(spot, group), place
                )
            places.append(place)
        for slot in range(group):
            found = jnp.int32(0)
            for source in range(group):
                found = jnp.where(places[source] == slot, source, found)
            slot_of.append(found)

    for step in order:
        for shift in range(halves):
            if step or shift:
                source = lax.rem(tile + step, tiles) * halves + lax.rem(half + shift, halves)
                pltpu.make_async_remote_copy(
                    src_ref=sar_send.at[0, 0],
                    dst_ref=arrived.at[source],
                    send_sem=sar_ssem.at[0],
                    recv_sem=sar_rsem.at[source],
                    device_id={"half": other_half},
                    device_id_type=MESH,
                ).wait_recv()
    per_patch = group // patch_dev
    for run in range(halves):
        for slot in range(group):
            at = run * quarter + (slot % per_patch) * lines
            sar_cols[slot // per_patch, at : at + lines, :] = arrived[slot_of[run * group + slot], run]

    loads[3].wait()
    for patch in range(patch_dev):
        for c in range(chunks):
            sar_rows[patch, c] = jnp.dot(
                row_v[c], sar_cols[patch], preferred_element_type=jnp.float32
            )

    lane = lax.broadcasted_iota(jnp.int32, (chunk, width), 1)
    line = lax.broadcasted_iota(jnp.int32, (chunk, width), 0)
    shared = (lane + half) == 0
    centre = (lane + line + half) == 0

    def parts(table_rows, first):
        a, c = table_rows[:chunk, :width], table_rows[:chunk, width:]
        b, d = table_rows[chunk:, :width], table_rows[chunk:, width:]
        if first:
            a = jnp.where(centre, 0.0, a)
        return a, b, c, d

    def cross_chunk(turn, patch, c):
        oa, ob, oc, od = parts(
            jnp.dot(row_v[c], opt_cols[turn], preferred_element_type=jnp.float32), c == 0
        )
        sa, sb, sc, sd = parts(sar_rows[patch, c], c == 0)
        o_re, o_im, s_re, s_im = oa + od, oc - ob, sa + sd, sc - sb
        real = o_re * s_re + o_im * s_im
        imag = o_re * s_im - o_im * s_re
        shared_real = oa * sa + ob * sb - (od * sc - oc * sd)
        shared_imag = ob * sa - oa * sb + (oc * sc + od * sd)
        real = jnp.where(shared, shared_real, real)
        imag = jnp.where(shared, shared_imag, imag)
        o_energy = jnp.sum(o_re * o_re + o_im * o_im, axis=0, keepdims=True)
        s_energy = jnp.sum(s_re * s_re + s_im * s_im, axis=0, keepdims=True)
        return real, imag, o_energy, s_energy

    weight = jnp.where(shared[:1], 1.0, 2.0)

    def pair_copy(k, src, dst, axis, to):
        return pltpu.make_async_remote_copy(
            src_ref=src,
            dst_ref=dst,
            send_sem=pair_ssem.at[k],
            recv_sem=pair_rsem.at[k],
            device_id={axis: to},
            device_id_type=MESH,
        )

    opt_copies[0].wait_recv()
    o_sum, s_sum = 0.0, 0.0
    for c in range(chunks):
        real, imag, o_energy, s_energy = cross_chunk(0, other_band, c)
        cross_send[c, :, :width] = real.astype(jnp.bfloat16)
        cross_send[c, :, width:] = imag.astype(jnp.bfloat16)
        o_sum, s_sum = o_sum + o_energy, s_sum + s_energy
    stat_send[0:1, :] = o_sum * weight
    stat_send[1:2, :] = s_sum * weight
    stat_send[2:8, :] = jnp.zeros((6, width), jnp.float32)
    cross_copy = pair_copy(0, cross_send, cross_recv, "band", other_band)
    cross_copy.start()
    stat_copy = pair_copy(1, stat_send, stat_recv, "band", other_band)
    stat_copy.start()

    opt_copies[1].wait_recv()
    o_sum, s_sum = 0.0, 0.0
    for c in range(chunks):
        real, imag, o_energy, s_energy = cross_chunk(1, band, c)
        cross_own[c, :, :width] = real
        cross_own[c, :, width:] = imag
        o_sum, s_sum = o_sum + o_energy, s_sum + s_energy

    cross_copy.wait_recv()
    for c in range(chunks):
        total = cross_own[c] + cross_recv[c].astype(jnp.float32)
        cross_all[c * chunk : (c + 1) * chunk, :] = total.astype(jnp.bfloat16)

    loads[4].wait()

    def lag_chunk(c):
        both = jnp.dot(row_v[c], cross_all[...], preferred_element_type=jnp.float32)
        lags[c, :, :width] = (both[:chunk, :width] - both[chunk:, width:]).astype(jnp.bfloat16)
        lags[c, :, width:] = (both[:chunk, width:] + both[chunk:, :width]).astype(jnp.bfloat16)

    for i in range(per_half):
        lag_chunk(other_half * per_half + i)
    lag_copy = pair_copy(2, lags.at[pl.ds(other_half * per_half, per_half)], lag_recv, "half", other_half)
    lag_copy.start()
    for i in range(per_half):
        lag_chunk(half * per_half + i)

    spots = lax.broadcasted_iota(jnp.int32, (peak_count, extent), 1)
    ranks = lax.broadcasted_iota(jnp.int32, (peak_count, extent), 0)

    def one_hot(which):
        wanted = jnp.zeros((peak_count, extent), jnp.int32)
        for j in range(peak_count):
            wanted = jnp.where(ranks == j, peaks_ref[0, which, j], wanted)
        return jnp.where(spots == wanted, 1.0, 0.0).astype(jnp.bfloat16)

    picked = jnp.dot(
        one_hot(0), lags[...].reshape(extent, 2 * width), preferred_element_type=jnp.float32
    )
    waves = lax.dot_general(
        one_hot(1), lag_v[half], (((1,), (1,)), ((), ())), preferred_element_type=jnp.float32
    )
    stat_copy.wait_recv()
    last_send[0:8, :] = stat_recv[...]
    last_send[0:1, :] = o_sum * weight + stat_recv[0:1, :]
    last_send[1:2, :] = s_sum * weight + stat_recv[1:2, :]
    last_send[8 : 8 + peak_count, :] = jnp.broadcast_to(
        jnp.sum(picked * waves, axis=1, keepdims=True), (peak_count, width)
    )
    last_copy = pair_copy(3, last_send, last_recv, "half", other_half)
    last_copy.start()

    own_lags = lags[pl.ds(half * per_half, per_half)].reshape(quarter, 2 * width)
    surface_ref[0] = jnp.dot(own_lags, lag_v[half], preferred_element_type=jnp.float32)

    last_copy.wait_recv()
    totals = last_send[...] + last_recv[...]
    pixels = extent * extent
    o_all = jnp.sum(totals[0:1, :], axis=1, keepdims=True) / (float(pixels) * bands * pixels)
    s_all = jnp.sum(totals[1:2, :], axis=1, keepdims=True) / (float(pixels) * bands * pixels)
    norm = lax.rsqrt(bands * pixels * (o_all + EPSILON) * (s_all + EPSILON)) / pixels
    peak_ref[...] = totals[8 : 8 + peak_count, :] * norm

    lag_copy.wait_recv()
    far = jnp.dot(
        lag_recv[...].reshape(quarter, 2 * width),
        lag_v[other_half],
        preferred_element_type=jnp.float32,
    )
    surface_ref[0] = (surface_ref[0] + far) * norm

    for copy in copies + opt_copies + [cross_copy, stat_copy, lag_copy, last_copy]:
        copy.wait_send()


def fused(mesh, optical, sar, destination, peaks):
    tiles, halves, bands = mesh.shape["tile"], mesh.shape["half"], mesh.shape["band"]
    patch_dev, _, quarter, extent = optical.shape
    group = tiles * halves
    lines = sar.shape[1] // group
    peak_count = peaks.shape[2]
    chunk = quarter // 2
    chunks = extent // chunk
    width = extent // 2 // halves
    sizes = (tiles, halves, bands, patch_dev, quarter, extent, lines, chunk, peak_count)
    tables = half_tables(extent, halves, chunk)
    bf, f32 = jnp.bfloat16, jnp.float32
    wide = 2 * width
    vmem = pltpu.VMEM
    dma = pltpu.SemaphoreType.DMA
    surface, peak_rows = pl.pallas_call(
        functools.partial(kernel, sizes),
        out_shape=(
            jax.ShapeDtypeStruct((1, quarter, extent), f32),
            jax.ShapeDtypeStruct((peak_count, width), f32),
        ),
        in_specs=[pl.BlockSpec(memory_space=pltpu.SMEM)] * 2
        + [pl.BlockSpec(memory_space=pl.ANY)] * 5,
        out_specs=(pl.BlockSpec(memory_space=pltpu.VMEM), pl.BlockSpec(memory_space=pltpu.VMEM)),
        scratch_shapes=[
            vmem((group, lines, extent), bf),
            vmem((patch_dev, quarter, extent), bf),
            vmem((extent, extent), bf),
            vmem((chunks, 2 * chunk, extent), bf),
            vmem((halves, wide, extent), bf),
            vmem((tiles, halves, halves, lines, wide), bf),
            vmem((group, halves, lines, wide), bf),
            vmem((patch_dev, halves, quarter, wide), bf),
            vmem((patch_dev, extent, wide), bf),
            vmem((patch_dev, extent, wide), bf),
            vmem((patch_dev, chunks, 2 * chunk, wide), f32),
            vmem((chunks, chunk, wide), bf),
            vmem((chunks, chunk, wide), bf),
            vmem((chunks, chunk, wide), f32),
            vmem((extent, wide), bf),
            vmem((8, width), f32),
            vmem((8, width), f32),
            vmem((8 + peak_count, width), f32),
            vmem((8 + peak_count, width), f32),
            vmem((chunks, chunk, wide), bf),
            vmem((chunks // halves, chunk, wide), bf),
            dma((5,)),
            dma((group,)),
            dma((group,)),
            dma((2,)),
            dma((2,)),
            dma((4,)),
            dma((4,)),
        ],
        compiler_params=pltpu.CompilerParams(
            collective_id=0, has_side_effects=True, vmem_limit_bytes=50 * 1024 * 1024
        ),
    )(
        destination,
        peaks,
        sar.reshape(group, lines, extent),
        optical.reshape(patch_dev, quarter, extent),
        *[jnp.asarray(t) for t in tables],
    )
    return surface, peak_rows[:, 0].reshape(1, peak_count)


def fits(mesh, optical, sar, peaks):
    group = mesh.shape["tile"] * mesh.shape["half"]
    patch_dev, local_bands, quarter, extent = optical.shape
    lines = sar.shape[1] // group
    return (
        mesh.shape["half"] == 2
        and mesh.shape["band"] == 2
        and patch_dev == 2
        and local_bands == 1
        and lines % 16 == 0
        and quarter % lines == 0
        and extent % 512 == 0
        and peaks.shape[0] == 1
        and peaks.shape[2] % 8 == 0
    )


def solution(mesh):
    def local(optical, sar, destination, peaks):
        if fits(mesh, optical, sar, peaks):
            return fused(mesh, optical, sar, destination, peaks)
        return generic(optical, sar, destination, peaks)

    in_specs = (
        P(("scene", "tile"), "band", "half", None),
        P("band", ("scene", "tile", "half"), None),
        P("scene"),
        P(("scene", "tile", "band"), None, None),
    )
    out_specs = (P(("scene", "tile", "band"), "half", None), P(("scene", "tile", "band"), None))
    return jax.shard_map(local, mesh=mesh, in_specs=in_specs, out_specs=out_specs, check_vma=False)
```

```python
import functools
import math

import jax
import jax.numpy as jnp
import numpy as np
from jax import lax
from jax.experimental import pallas as pl
from jax.experimental.pallas import tpu as pltpu
from jax.sharding import PartitionSpec as P

MESH = pl.DeviceIdType.MESH

precise = lax.Precision.HIGHEST
EPSILON = 1e-06


def fourier_tables(extent):
    places = jnp.arange(extent, dtype=jnp.int32)
    phases = places[:, None] * places[None, :] % extent
    angles = phases.astype(jnp.float32) * (2.0 * math.pi / extent)
    return (jnp.cos(angles), jnp.sin(angles))


def fourier_pair(table):
    upper = table.astype(jnp.bfloat16)
    lower = (table - upper.astype(jnp.float32)).astype(jnp.bfloat16)
    return (upper, lower)


def column_spectrum(samples, table_upper, table_lower):
    extent = samples.shape[-1]
    values = samples.reshape(-1, extent)
    spectrum = jnp.dot(values, table_upper, preferred_element_type=jnp.float32) + jnp.dot(
        values, table_lower, preferred_element_type=jnp.float32
    )
    return spectrum.astype(jnp.bfloat16).reshape(samples.shape[:-1] + (2 * extent,))


def row_spectrum(columns, table_upper, table_lower):
    line_count = columns.shape[-3]
    stacked = jnp.concatenate([columns[..., 0, :], columns[..., 1, :]], axis=-2)
    result = jnp.einsum("kr,...rc->...kc", table_upper, stacked, preferred_element_type=jnp.float32)
    result = result + jnp.einsum(
        "kr,...rc->...kc", table_lower, stacked, preferred_element_type=jnp.float32
    )
    return (result[..., :line_count, :], result[..., line_count:, :])


def relay_blocks(parcel):
    layout = parcel.shape
    merged = parcel.reshape(layout[:1] + (layout[1] * layout[2],) + layout[3:])
    arrived = lax.all_to_all(merged, ("tile", "half"), split_axis=1, concat_axis=1, tiled=True)
    return arrived.reshape(layout)


def generic(optical, sar, destination, peaks):
    tile_count = lax.axis_size("tile")
    half_count = lax.axis_size("half")
    band_count = lax.axis_size("band")
    group_size = tile_count * half_count
    patch_dev, local_bands, quarter, extent = optical.shape
    col_width = extent // half_count
    block_lines = sar.shape[1] // group_size
    band_total = local_bands * band_count
    pixel_count = extent * extent
    patch_total = patch_dev * tile_count
    kept_patches = patch_dev // band_count
    cosine_table, sine_table = fourier_tables(extent)
    col_upper, col_lower = fourier_pair(jnp.concatenate([cosine_table, -sine_table], axis=1))
    row_full = jnp.concatenate(
        [
            jnp.concatenate([cosine_table, sine_table], axis=1),
            jnp.concatenate([-sine_table, cosine_table], axis=1),
        ],
        axis=0,
    )
    row_upper, row_lower = fourier_pair(row_full)
    tile_at = lax.axis_index("tile")
    half_at = lax.axis_index("half")
    band_at = lax.axis_index("band")
    device_at = lax.axis_index(("tile", "half"))
    own_blocks = lax.dynamic_slice_in_dim(destination, device_at * group_size, group_size)
    send_order = jnp.argsort(own_blocks // group_size)
    inverse = (
        jnp.zeros_like(destination)
        .at[destination]
        .set(jnp.arange(destination.shape[0], dtype=jnp.int32))
    )
    opt_values = optical.astype(jnp.float32)
    opt_sums = jnp.sum(opt_values, axis=(2, 3))
    opt_squares = jnp.sum(opt_values * opt_values, axis=(2, 3))
    sar_values = sar.astype(jnp.float32).reshape(local_bands, group_size, block_lines * extent)
    sar_sums = jnp.sum(sar_values, axis=2)
    sar_squares = jnp.sum(sar_values * sar_values, axis=2)
    map_device = own_blocks // group_size
    map_patch = (
        map_device // half_count * patch_dev + own_blocks % group_size * block_lines // quarter
    )
    member = (map_patch[:, None] == jnp.arange(patch_total, dtype=jnp.int32)[None, :]).astype(
        jnp.float32
    )
    sar_stats = jnp.dot(
        jnp.stack([sar_sums, sar_squares]).reshape(2 * local_bands, group_size),
        member,
        precision=precise,
        preferred_element_type=jnp.float32,
    )
    statistics = jnp.zeros((2, 2, band_total, patch_total), jnp.float32)
    opt_part = jnp.transpose(jnp.stack([opt_sums, opt_squares]), (0, 2, 1))
    statistics = lax.dynamic_update_slice(
        statistics, opt_part[None], (0, 0, band_at * local_bands, tile_at * patch_dev)
    )
    statistics = lax.dynamic_update_slice(
        statistics,
        sar_stats.reshape(2, local_bands, patch_total)[None],
        (1, 0, band_at * local_bands, 0),
    )
    totals = lax.psum(statistics, ("tile", "half", "band"))
    centered = totals[:, 1] - totals[:, 0] * totals[:, 0] / pixel_count
    energy = jnp.sum(centered, axis=1) / (band_total * pixel_count)
    norm_scale = lax.rsqrt(band_total * pixel_count * (energy[0] + EPSILON) * (energy[1] + EPSILON))
    first_patch = tile_at * patch_dev + band_at * kept_patches
    norm_mine = lax.dynamic_slice_in_dim(norm_scale, first_patch, kept_patches)
    slant_spectra = column_spectrum(sar, col_upper, col_lower).reshape(
        local_bands, group_size, block_lines, 2, half_count, col_width
    )
    outgoing = jnp.take(slant_spectra, send_order, axis=1).reshape(
        local_bands, tile_count, half_count, block_lines, 2, half_count, col_width
    )
    outgoing = jnp.transpose(outgoing, (0, 1, 5, 2, 3, 4, 6))
    arrived = relay_blocks(outgoing).reshape(
        local_bands, group_size * half_count, block_lines, 2, col_width
    )
    sources = lax.dynamic_slice_in_dim(
        inverse, tile_at * half_count * group_size, half_count * group_size
    )
    slot_index = (
        sources // group_size * half_count
        + jnp.arange(half_count * group_size, dtype=jnp.int32) // group_size
    )
    placed = jnp.take(arrived, slot_index, axis=1).reshape(
        local_bands, half_count, patch_dev, quarter, 2, col_width
    )
    placed = jnp.transpose(placed, (2, 0, 1, 3, 4, 5)).reshape(
        patch_dev, local_bands, extent, 2, col_width
    )
    sar_real, sar_imag = row_spectrum(placed, row_upper, row_lower)
    spectra = column_spectrum(optical, col_upper, col_lower).reshape(
        patch_dev, local_bands, quarter, 2, half_count, col_width
    )
    real_part, imag_part = row_spectrum(
        jnp.squeeze(
            lax.all_to_all(spectra, "half", split_axis=4, concat_axis=2, tiled=True), axis=4
        ),
        row_upper,
        row_lower,
    )
    opt_real = real_part
    opt_imag = imag_part
    rows_at = jnp.arange(extent, dtype=jnp.int32)[:, None]
    cols_at = half_at * col_width + jnp.arange(col_width, dtype=jnp.int32)[None, :]
    keep_mask = jnp.where((rows_at == 0) & (cols_at == 0), 0.0, 1.0).astype(jnp.float32)
    opt_real = opt_real * keep_mask
    opt_imag = opt_imag * keep_mask
    sar_real = sar_real * keep_mask
    sar_imag = sar_imag * keep_mask
    cross_real = jnp.sum(opt_real * sar_real + opt_imag * sar_imag, axis=1)
    cross_imag = jnp.sum(opt_real * sar_imag - opt_imag * sar_real, axis=1)
    cross_term = jnp.stack([cross_real, cross_imag], axis=1)
    cross_sum = lax.psum_scatter(cross_term, "band", scatter_dimension=0, tiled=True)
    lag_real = (
        jnp.einsum("uk,pkc->puc", cosine_table, cross_sum[:, 0], precision=precise)
        - jnp.einsum("uk,pkc->puc", sine_table, cross_sum[:, 1], precision=precise)
    ) / extent
    lag_imag = (
        jnp.einsum("uk,pkc->puc", cosine_table, cross_sum[:, 1], precision=precise)
        + jnp.einsum("uk,pkc->puc", sine_table, cross_sum[:, 0], precision=precise)
    ) / extent
    lagged = jnp.stack([lag_real, lag_imag], axis=2).reshape(
        kept_patches, half_count, quarter, 2, col_width
    )
    pieces = lax.all_to_all(lagged, "half", split_axis=1, concat_axis=4, tiled=True)
    real_in = pieces[:, 0, :, 0, :]
    imag_in = pieces[:, 0, :, 1, :]
    correlation = (
        jnp.einsum("puc,cv->puv", real_in, cosine_table, precision=precise)
        - jnp.einsum("puc,cv->puv", imag_in, sine_table, precision=precise)
    ) / extent
    surface = correlation * norm_mine[:, None, None]
    local_rows = peaks[:, 0, :] - half_at * quarter
    row_hit = (
        local_rows[:, :, None] == jnp.arange(quarter, dtype=jnp.int32)[None, None, :]
    ).astype(jnp.float32)
    picked = jnp.einsum("pkr,prc->pkc", row_hit, surface, precision=precise)
    col_hit = (peaks[:, 1, :, None] == jnp.arange(extent, dtype=jnp.int32)[None, None, :]).astype(
        jnp.float32
    )
    local_values = jnp.sum(picked * col_hit, axis=2)
    peak_values = lax.psum(local_values, "half")
    return (surface, peak_values)


def half_tables(extent, half_count, chunk):
    width = extent // 2 // half_count
    places = np.arange(extent)
    phases = (places[:, None] * places[None, :]) % extent
    cosine = np.cos(phases * (2.0 * np.pi / extent))
    sine = np.sin(phases * (2.0 * np.pi / extent))
    forward, backward = [], []
    for half in range(half_count):
        span = slice(half * width, (half + 1) * width)
        real, imag = cosine[:, span].copy(), -sine[:, span]
        real_back, imag_back = 2.0 * cosine[span], -2.0 * sine[span]
        if half == 0:
            imag[:, 0] = cosine[:, extent // 2]
            real_back[0] = 1.0
            imag_back[0] = cosine[extent // 2]
        forward.append(np.concatenate([real, imag], axis=1))
        backward.append(np.concatenate([real_back, imag_back], axis=0))
    col_table = np.concatenate(forward, axis=1)
    lag_table = np.stack(backward)
    row_table = np.concatenate(
        [cosine.reshape(-1, chunk, extent), sine.reshape(-1, chunk, extent)], axis=1
    )
    return tuple(t.astype(jnp.bfloat16) for t in (col_table, row_table, lag_table))


def kernel(
    sizes,
    dest_hbm,
    peaks_hbm,
    sar_hbm,
    opt_hbm,
    col_hbm,
    row_hbm,
    lag_hbm,
    surface_ref,
    peak_ref,
    dest_ref,
    peaks_ref,
    sar_v,
    opt_v,
    col_v,
    row_v,
    lag_v,
    sar_send,
    arrived,
    opt_send,
    opt_cols,
    sar_cols,
    sar_rows,
    cross_send,
    cross_recv,
    cross_own,
    cross_all,
    stat_send,
    stat_recv,
    last_send,
    last_recv,
    lags,
    lag_recv,
    load_sem,
    sar_ssem,
    sar_rsem,
    opt_ssem,
    opt_rsem,
    pair_ssem,
    pair_rsem,
):
    tiles, halves, bands, patch_dev, quarter, extent, lines, chunk, peak_count = sizes
    group = tiles * halves
    width = extent // 2 // halves
    chunks = extent // chunk
    per_half = chunks // halves
    tile, half, band = lax.axis_index("tile"), lax.axis_index("half"), lax.axis_index("band")
    me = tile * halves + half
    other_half = 1 - half
    other_band = 1 - band

    loads = [
        pltpu.make_async_copy(a, b, load_sem.at[i])
        for i, (a, b) in enumerate(
            [(sar_hbm, sar_v), (col_hbm, col_v), (opt_hbm, opt_v), (row_hbm, row_v), (lag_hbm, lag_v),
             (dest_hbm, dest_ref), (peaks_hbm, peaks_ref)]
        )
    ]
    for load in loads:
        load.start()

    barrier = pltpu.get_barrier_semaphore()
    for step in range(tiles):
        for shift in range(halves):
            if step or shift:
                pl.semaphore_signal(
                    barrier,
                    inc=1,
                    device_id={
                        "tile": lax.rem(tile + step, tiles),
                        "half": lax.rem(half + shift, halves),
                    },
                    device_id_type=MESH,
                )
    pl.semaphore_signal(barrier, inc=1, device_id={"band": other_band}, device_id_type=MESH)

    loads[5].wait()
    own_runs = [lax.div(dest_ref[me * group + j], group) for j in range(group)]

    def block_for(run):
        found = jnp.int32(0)
        for j in range(group):
            found = jnp.where(own_runs[j] == run, j, found)
        return found

    loads[0].wait()
    loads[1].wait()
    pl.semaphore_wait(barrier, group)

    def sar_copy(step, shift):
        to_half = lax.rem(half + shift, halves)
        return pltpu.make_async_remote_copy(
            src_ref=sar_send.at[step, to_half],
            dst_ref=arrived.at[me],
            send_sem=sar_ssem.at[step * halves + shift],
            recv_sem=sar_rsem.at[me],
            device_id={"tile": lax.rem(tile + step, tiles), "half": to_half},
            device_id_type=MESH,
        )

    copies = []
    order = sorted(range(tiles), key=lambda s: -min(s, tiles - s))
    for step in order:
        to_tile = lax.rem(tile + step, tiles)
        samples = jnp.concatenate(
            [sar_v[block_for(to_tile * halves + run)] for run in range(halves)], axis=0
        )
        spectra = jnp.dot(samples, col_v[...], preferred_element_type=jnp.float32)
        spectra = spectra.astype(jnp.bfloat16)
        for to_half in range(halves):
            piece = spectra[:, to_half * 2 * width : (to_half + 1) * 2 * width]
            sar_send[step, to_half] = piece.reshape(halves, lines, 2 * width)
        for shift in reversed(range(halves)):
            if step or shift:
                copy = sar_copy(step, shift)
                copy.start()
                copies.append(copy)
    arrived[me] = sar_send[0, half]

    opt_copies = []
    loads[2].wait()
    for turn, patch in enumerate((other_band, band)):
        spectra = jnp.dot(opt_v[patch], col_v[...], preferred_element_type=jnp.float32)
        spectra = spectra.astype(jnp.bfloat16)
        for to_half in range(halves):
            opt_send[turn, to_half] = spectra[:, to_half * 2 * width : (to_half + 1) * 2 * width]
        rows = pl.ds(pl.multiple_of(half * quarter, quarter), quarter)
        copy = pltpu.make_async_remote_copy(
            src_ref=opt_send.at[turn, other_half],
            dst_ref=opt_cols.at[turn, rows],
            send_sem=opt_ssem.at[turn],
            recv_sem=opt_rsem.at[turn],
            device_id={"half": other_half},
            device_id_type=MESH,
        )
        copy.start()
        opt_copies.append(copy)
        opt_cols[turn, rows, :] = opt_send[turn, half]

    slot_of = []
    for run in range(halves):
        places = []
        for source in range(group):
            place = jnp.int32(0)
            for j in range(group):
                spot = dest_ref[source * group + j]
                place = jnp.where(
                    lax.div(spot, group) == tile * halves + run, lax.rem(spot, group), place
                )
            places.append(place)
        for slot in range(group):
            found = jnp.int32(0)
            for source in range(group):
                found = jnp.where(places[source] == slot, source, found)
            slot_of.append(found)

    for step in order:
        for shift in range(halves):
            if step or shift:
                source = lax.rem(tile + step, tiles) * halves + lax.rem(half + shift, halves)
                pltpu.make_async_remote_copy(
                    src_ref=sar_send.at[0, 0],
                    dst_ref=arrived.at[source],
                    send_sem=sar_ssem.at[0],
                    recv_sem=sar_rsem.at[source],
                    device_id={"half": other_half},
                    device_id_type=MESH,
                ).wait_recv()
    per_patch = group // patch_dev
    for run in range(halves):
        for slot in range(group):
            at = run * quarter + (slot % per_patch) * lines
            sar_cols[slot // per_patch, at : at + lines, :] = arrived[slot_of[run * group + slot], run]

    loads[3].wait()
    for patch in range(patch_dev):
        for c in range(chunks):
            sar_rows[patch, c] = jnp.dot(
                row_v[c], sar_cols[patch], preferred_element_type=jnp.float32
            )

    lane = lax.broadcasted_iota(jnp.int32, (chunk, width), 1)
    line = lax.broadcasted_iota(jnp.int32, (chunk, width), 0)
    shared = (lane + half) == 0
    centre = (lane + line + half) == 0

    def parts(table_rows, first):
        a, c = table_rows[:chunk, :width], table_rows[:chunk, width:]
        b, d = table_rows[chunk:, :width], table_rows[chunk:, width:]
        if first:
            a = jnp.where(centre, 0.0, a)
        return a, b, c, d

    def cross_chunk(turn, patch, c):
        oa, ob, oc, od = parts(
            jnp.dot(row_v[c], opt_cols[turn], preferred_element_type=jnp.float32), c == 0
        )
        sa, sb, sc, sd = parts(sar_rows[patch, c], c == 0)
        o_re, o_im, s_re, s_im = oa + od, oc - ob, sa + sd, sc - sb
        real = o_re * s_re + o_im * s_im
        imag = o_re * s_im - o_im * s_re
        shared_real = oa * sa + ob * sb - (od * sc - oc * sd)
        shared_imag = ob * sa - oa * sb + (oc * sc + od * sd)
        real = jnp.where(shared, shared_real, real)
        imag = jnp.where(shared, shared_imag, imag)
        o_energy = jnp.sum(o_re * o_re + o_im * o_im, axis=0, keepdims=True)
        s_energy = jnp.sum(s_re * s_re + s_im * s_im, axis=0, keepdims=True)
        return real, imag, o_energy, s_energy

    weight = jnp.where(shared[:1], 1.0, 2.0)

    def pair_copy(k, src, dst, axis, to):
        return pltpu.make_async_remote_copy(
            src_ref=src,
            dst_ref=dst,
            send_sem=pair_ssem.at[k],
            recv_sem=pair_rsem.at[k],
            device_id={axis: to},
            device_id_type=MESH,
        )

    opt_copies[0].wait_recv()
    o_sum, s_sum = 0.0, 0.0
    for c in range(chunks):
        real, imag, o_energy, s_energy = cross_chunk(0, other_band, c)
        cross_send[c, :, :width] = real.astype(jnp.bfloat16)
        cross_send[c, :, width:] = imag.astype(jnp.bfloat16)
        o_sum, s_sum = o_sum + o_energy, s_sum + s_energy
    stat_send[0:1, :] = o_sum * weight
    stat_send[1:2, :] = s_sum * weight
    stat_send[2:8, :] = jnp.zeros((6, width), jnp.float32)
    cross_copy = pair_copy(0, cross_send, cross_recv, "band", other_band)
    cross_copy.start()
    stat_copy = pair_copy(1, stat_send, stat_recv, "band", other_band)
    stat_copy.start()

    opt_copies[1].wait_recv()
    o_sum, s_sum = 0.0, 0.0
    for c in range(chunks):
        real, imag, o_energy, s_energy = cross_chunk(1, band, c)
        cross_own[c, :, :width] = real
        cross_own[c, :, width:] = imag
        o_sum, s_sum = o_sum + o_energy, s_sum + s_energy

    cross_copy.wait_recv()
    for c in range(chunks):
        total = cross_own[c] + cross_recv[c].astype(jnp.float32)
        cross_all[c * chunk : (c + 1) * chunk, :] = total.astype(jnp.bfloat16)

    loads[4].wait()

    def lag_chunk(c):
        both = jnp.dot(row_v[c], cross_all[...], preferred_element_type=jnp.float32)
        lags[c, :, :width] = (both[:chunk, :width] - both[chunk:, width:]).astype(jnp.bfloat16)
        lags[c, :, width:] = (both[:chunk, width:] + both[chunk:, :width]).astype(jnp.bfloat16)

    for i in range(per_half):
        lag_chunk(other_half * per_half + i)
    lag_copy = pair_copy(2, lags.at[pl.ds(other_half * per_half, per_half)], lag_recv, "half", other_half)
    lag_copy.start()
    for i in range(per_half):
        lag_chunk(half * per_half + i)

    spots = lax.broadcasted_iota(jnp.int32, (peak_count, extent), 1)
    ranks = lax.broadcasted_iota(jnp.int32, (peak_count, extent), 0)

    loads[6].wait()

    def one_hot(which):
        wanted = jnp.zeros((peak_count, extent), jnp.int32)
        for j in range(peak_count):
            wanted = jnp.where(ranks == j, peaks_ref[0, which, j], wanted)
        return jnp.where(spots == wanted, 1.0, 0.0).astype(jnp.bfloat16)

    picked = jnp.dot(
        one_hot(0), lags[...].reshape(extent, 2 * width), preferred_element_type=jnp.float32
    )
    waves = lax.dot_general(
        one_hot(1), lag_v[half], (((1,), (1,)), ((), ())), preferred_element_type=jnp.float32
    )
    stat_copy.wait_recv()
    last_send[0:8, :] = stat_recv[...]
    last_send[0:1, :] = o_sum * weight + stat_recv[0:1, :]
    last_send[1:2, :] = s_sum * weight + stat_recv[1:2, :]
    last_send[8 : 8 + peak_count, :] = jnp.broadcast_to(
        jnp.sum(picked * waves, axis=1, keepdims=True), (peak_count, width)
    )
    last_copy = pair_copy(3, last_send, last_recv, "half", other_half)
    last_copy.start()

    own_lags = lags[pl.ds(half * per_half, per_half)].reshape(quarter, 2 * width)
    surface_ref[0] = jnp.dot(own_lags, lag_v[half], preferred_element_type=jnp.float32)

    last_copy.wait_recv()
    totals = last_send[...] + last_recv[...]
    pixels = extent * extent
    o_all = jnp.sum(totals[0:1, :], axis=1, keepdims=True) / (float(pixels) * bands * pixels)
    s_all = jnp.sum(totals[1:2, :], axis=1, keepdims=True) / (float(pixels) * bands * pixels)
    norm = lax.rsqrt(bands * pixels * (o_all + EPSILON) * (s_all + EPSILON)) / pixels
    peak_ref[...] = totals[8 : 8 + peak_count, :] * norm

    lag_copy.wait_recv()
    far = jnp.dot(
        lag_recv[...].reshape(quarter, 2 * width),
        lag_v[other_half],
        preferred_element_type=jnp.float32,
    )
    surface_ref[0] = (surface_ref[0] + far) * norm

    for copy in copies + opt_copies + [cross_copy, stat_copy, lag_copy, last_copy]:
        copy.wait_send()


def fused(mesh, optical, sar, destination, peaks):
    tiles, halves, bands = mesh.shape["tile"], mesh.shape["half"], mesh.shape["band"]
    patch_dev, _, quarter, extent = optical.shape
    group = tiles * halves
    lines = sar.shape[1] // group
    peak_count = peaks.shape[2]
    chunk = quarter // 2
    chunks = extent // chunk
    width = extent // 2 // halves
    sizes = (tiles, halves, bands, patch_dev, quarter, extent, lines, chunk, peak_count)
    tables = half_tables(extent, halves, chunk)
    bf, f32 = jnp.bfloat16, jnp.float32
    wide = 2 * width
    vmem = pltpu.VMEM
    dma = pltpu.SemaphoreType.DMA
    surface, peak_rows = pl.pallas_call(
        functools.partial(kernel, sizes),
        out_shape=(
            jax.ShapeDtypeStruct((1, quarter, extent), f32),
            jax.ShapeDtypeStruct((peak_count, width), f32),
        ),
        in_specs=[pl.BlockSpec(memory_space=pltpu.HBM)] * 7,
        out_specs=(pl.BlockSpec(memory_space=pltpu.VMEM), pl.BlockSpec(memory_space=pltpu.VMEM)),
        scratch_shapes=[
            pltpu.SMEM(destination.shape, jnp.int32),
            pltpu.SMEM(peaks.shape, jnp.int32),
            vmem((group, lines, extent), bf),
            vmem((patch_dev, quarter, extent), bf),
            vmem((extent, extent), bf),
            vmem((chunks, 2 * chunk, extent), bf),
            vmem((halves, wide, extent), bf),
            vmem((tiles, halves, halves, lines, wide), bf),
            vmem((group, halves, lines, wide), bf),
            vmem((patch_dev, halves, quarter, wide), bf),
            vmem((patch_dev, extent, wide), bf),
            vmem((patch_dev, extent, wide), bf),
            vmem((patch_dev, chunks, 2 * chunk, wide), f32),
            vmem((chunks, chunk, wide), bf),
            vmem((chunks, chunk, wide), bf),
            vmem((chunks, chunk, wide), f32),
            vmem((extent, wide), bf),
            vmem((8, width), f32),
            vmem((8, width), f32),
            vmem((8 + peak_count, width), f32),
            vmem((8 + peak_count, width), f32),
            vmem((chunks, chunk, wide), bf),
            vmem((chunks // halves, chunk, wide), bf),
            dma((7,)),
            dma((group,)),
            dma((group,)),
            dma((2,)),
            dma((2,)),
            dma((4,)),
            dma((4,)),
        ],
        compiler_params=pltpu.CompilerParams(
            collective_id=0, has_side_effects=True, vmem_limit_bytes=67000000
        ),
    )(
        destination,
        peaks,
        sar.reshape(group, lines, extent),
        optical.reshape(patch_dev, quarter, extent),
        *[jnp.asarray(t) for t in tables],
    )
    return surface, peak_rows[:, 0].reshape(1, peak_count)


def fits(mesh, optical, sar, peaks):
    group = mesh.shape["tile"] * mesh.shape["half"]
    patch_dev, local_bands, quarter, extent = optical.shape
    lines = sar.shape[1] // group
    return (
        mesh.shape["half"] == 2
        and mesh.shape["band"] == 2
        and patch_dev == 2
        and local_bands == 1
        and lines % 16 == 0
        and quarter % lines == 0
        and extent % 512 == 0
        and peaks.shape[0] == 1
        and peaks.shape[2] % 8 == 0
    )


def solution(mesh):
    def local(optical, sar, destination, peaks):
        if fits(mesh, optical, sar, peaks):
            return fused(mesh, optical, sar, destination, peaks)
        return generic(optical, sar, destination, peaks)

    in_specs = (
        P(("scene", "tile"), "band", "half", None),
        P("band", ("scene", "tile", "half"), None),
        P("scene"),
        P(("scene", "tile", "band"), None, None),
    )
    out_specs = (P(("scene", "tile", "band"), "half", None), P(("scene", "tile", "band"), None))
    return jax.shard_map(local, mesh=mesh, in_specs=in_specs, out_specs=out_specs, check_vma=False)
```

```python
import functools
import math

import jax
import jax.numpy as jnp
import numpy as np
from jax import lax
from jax.experimental import pallas as pl
from jax.experimental.pallas import tpu as pltpu
from jax.sharding import PartitionSpec as P

MESH = pl.DeviceIdType.MESH

precise = lax.Precision.HIGHEST
EPSILON = 1e-06


def fourier_tables(extent):
    places = jnp.arange(extent, dtype=jnp.int32)
    phases = places[:, None] * places[None, :] % extent
    angles = phases.astype(jnp.float32) * (2.0 * math.pi / extent)
    return (jnp.cos(angles), jnp.sin(angles))


def fourier_pair(table):
    upper = table.astype(jnp.bfloat16)
    lower = (table - upper.astype(jnp.float32)).astype(jnp.bfloat16)
    return (upper, lower)


def column_spectrum(samples, table_upper, table_lower):
    extent = samples.shape[-1]
    values = samples.reshape(-1, extent)
    spectrum = jnp.dot(values, table_upper, preferred_element_type=jnp.float32) + jnp.dot(
        values, table_lower, preferred_element_type=jnp.float32
    )
    return spectrum.astype(jnp.bfloat16).reshape(samples.shape[:-1] + (2 * extent,))


def row_spectrum(columns, table_upper, table_lower):
    line_count = columns.shape[-3]
    stacked = jnp.concatenate([columns[..., 0, :], columns[..., 1, :]], axis=-2)
    result = jnp.einsum("kr,...rc->...kc", table_upper, stacked, preferred_element_type=jnp.float32)
    result = result + jnp.einsum(
        "kr,...rc->...kc", table_lower, stacked, preferred_element_type=jnp.float32
    )
    return (result[..., :line_count, :], result[..., line_count:, :])


def relay_blocks(parcel):
    layout = parcel.shape
    merged = parcel.reshape(layout[:1] + (layout[1] * layout[2],) + layout[3:])
    arrived = lax.all_to_all(merged, ("tile", "half"), split_axis=1, concat_axis=1, tiled=True)
    return arrived.reshape(layout)


def generic(optical, sar, destination, peaks):
    tile_count = lax.axis_size("tile")
    half_count = lax.axis_size("half")
    band_count = lax.axis_size("band")
    group_size = tile_count * half_count
    patch_dev, local_bands, quarter, extent = optical.shape
    col_width = extent // half_count
    block_lines = sar.shape[1] // group_size
    band_total = local_bands * band_count
    pixel_count = extent * extent
    patch_total = patch_dev * tile_count
    kept_patches = patch_dev // band_count
    cosine_table, sine_table = fourier_tables(extent)
    col_upper, col_lower = fourier_pair(jnp.concatenate([cosine_table, -sine_table], axis=1))
    row_full = jnp.concatenate(
        [
            jnp.concatenate([cosine_table, sine_table], axis=1),
            jnp.concatenate([-sine_table, cosine_table], axis=1),
        ],
        axis=0,
    )
    row_upper, row_lower = fourier_pair(row_full)
    tile_at = lax.axis_index("tile")
    half_at = lax.axis_index("half")
    band_at = lax.axis_index("band")
    device_at = lax.axis_index(("tile", "half"))
    own_blocks = lax.dynamic_slice_in_dim(destination, device_at * group_size, group_size)
    send_order = jnp.argsort(own_blocks // group_size)
    inverse = (
        jnp.zeros_like(destination)
        .at[destination]
        .set(jnp.arange(destination.shape[0], dtype=jnp.int32))
    )
    opt_values = optical.astype(jnp.float32)
    opt_sums = jnp.sum(opt_values, axis=(2, 3))
    opt_squares = jnp.sum(opt_values * opt_values, axis=(2, 3))
    sar_values = sar.astype(jnp.float32).reshape(local_bands, group_size, block_lines * extent)
    sar_sums = jnp.sum(sar_values, axis=2)
    sar_squares = jnp.sum(sar_values * sar_values, axis=2)
    map_device = own_blocks // group_size
    map_patch = (
        map_device // half_count * patch_dev + own_blocks % group_size * block_lines // quarter
    )
    member = (map_patch[:, None] == jnp.arange(patch_total, dtype=jnp.int32)[None, :]).astype(
        jnp.float32
    )
    sar_stats = jnp.dot(
        jnp.stack([sar_sums, sar_squares]).reshape(2 * local_bands, group_size),
        member,
        precision=precise,
        preferred_element_type=jnp.float32,
    )
    statistics = jnp.zeros((2, 2, band_total, patch_total), jnp.float32)
    opt_part = jnp.transpose(jnp.stack([opt_sums, opt_squares]), (0, 2, 1))
    statistics = lax.dynamic_update_slice(
        statistics, opt_part[None], (0, 0, band_at * local_bands, tile_at * patch_dev)
    )
    statistics = lax.dynamic_update_slice(
        statistics,
        sar_stats.reshape(2, local_bands, patch_total)[None],
        (1, 0, band_at * local_bands, 0),
    )
    totals = lax.psum(statistics, ("tile", "half", "band"))
    centered = totals[:, 1] - totals[:, 0] * totals[:, 0] / pixel_count
    energy = jnp.sum(centered, axis=1) / (band_total * pixel_count)
    norm_scale = lax.rsqrt(band_total * pixel_count * (energy[0] + EPSILON) * (energy[1] + EPSILON))
    first_patch = tile_at * patch_dev + band_at * kept_patches
    norm_mine = lax.dynamic_slice_in_dim(norm_scale, first_patch, kept_patches)
    slant_spectra = column_spectrum(sar, col_upper, col_lower).reshape(
        local_bands, group_size, block_lines, 2, half_count, col_width
    )
    outgoing = jnp.take(slant_spectra, send_order, axis=1).reshape(
        local_bands, tile_count, half_count, block_lines, 2, half_count, col_width
    )
    outgoing = jnp.transpose(outgoing, (0, 1, 5, 2, 3, 4, 6))
    arrived = relay_blocks(outgoing).reshape(
        local_bands, group_size * half_count, block_lines, 2, col_width
    )
    sources = lax.dynamic_slice_in_dim(
        inverse, tile_at * half_count * group_size, half_count * group_size
    )
    slot_index = (
        sources // group_size * half_count
        + jnp.arange(half_count * group_size, dtype=jnp.int32) // group_size
    )
    placed = jnp.take(arrived, slot_index, axis=1).reshape(
        local_bands, half_count, patch_dev, quarter, 2, col_width
    )
    placed = jnp.transpose(placed, (2, 0, 1, 3, 4, 5)).reshape(
        patch_dev, local_bands, extent, 2, col_width
    )
    sar_real, sar_imag = row_spectrum(placed, row_upper, row_lower)
    spectra = column_spectrum(optical, col_upper, col_lower).reshape(
        patch_dev, local_bands, quarter, 2, half_count, col_width
    )
    real_part, imag_part = row_spectrum(
        jnp.squeeze(
            lax.all_to_all(spectra, "half", split_axis=4, concat_axis=2, tiled=True), axis=4
        ),
        row_upper,
        row_lower,
    )
    opt_real = real_part
    opt_imag = imag_part
    rows_at = jnp.arange(extent, dtype=jnp.int32)[:, None]
    cols_at = half_at * col_width + jnp.arange(col_width, dtype=jnp.int32)[None, :]
    keep_mask = jnp.where((rows_at == 0) & (cols_at == 0), 0.0, 1.0).astype(jnp.float32)
    opt_real = opt_real * keep_mask
    opt_imag = opt_imag * keep_mask
    sar_real = sar_real * keep_mask
    sar_imag = sar_imag * keep_mask
    cross_real = jnp.sum(opt_real * sar_real + opt_imag * sar_imag, axis=1)
    cross_imag = jnp.sum(opt_real * sar_imag - opt_imag * sar_real, axis=1)
    cross_term = jnp.stack([cross_real, cross_imag], axis=1)
    cross_sum = lax.psum_scatter(cross_term, "band", scatter_dimension=0, tiled=True)
    lag_real = (
        jnp.einsum("uk,pkc->puc", cosine_table, cross_sum[:, 0], precision=precise)
        - jnp.einsum("uk,pkc->puc", sine_table, cross_sum[:, 1], precision=precise)
    ) / extent
    lag_imag = (
        jnp.einsum("uk,pkc->puc", cosine_table, cross_sum[:, 1], precision=precise)
        + jnp.einsum("uk,pkc->puc", sine_table, cross_sum[:, 0], precision=precise)
    ) / extent
    lagged = jnp.stack([lag_real, lag_imag], axis=2).reshape(
        kept_patches, half_count, quarter, 2, col_width
    )
    pieces = lax.all_to_all(lagged, "half", split_axis=1, concat_axis=4, tiled=True)
    real_in = pieces[:, 0, :, 0, :]
    imag_in = pieces[:, 0, :, 1, :]
    correlation = (
        jnp.einsum("puc,cv->puv", real_in, cosine_table, precision=precise)
        - jnp.einsum("puc,cv->puv", imag_in, sine_table, precision=precise)
    ) / extent
    surface = correlation * norm_mine[:, None, None]
    local_rows = peaks[:, 0, :] - half_at * quarter
    row_hit = (
        local_rows[:, :, None] == jnp.arange(quarter, dtype=jnp.int32)[None, None, :]
    ).astype(jnp.float32)
    picked = jnp.einsum("pkr,prc->pkc", row_hit, surface, precision=precise)
    col_hit = (peaks[:, 1, :, None] == jnp.arange(extent, dtype=jnp.int32)[None, None, :]).astype(
        jnp.float32
    )
    local_values = jnp.sum(picked * col_hit, axis=2)
    peak_values = lax.psum(local_values, "half")
    return (surface, peak_values)


def half_tables(extent, half_count, chunk):
    width = extent // 2 // half_count
    places = np.arange(extent)
    phases = (places[:, None] * places[None, :]) % extent
    cosine = np.cos(phases * (2.0 * np.pi / extent))
    sine = np.sin(phases * (2.0 * np.pi / extent))
    forward, backward = [], []
    for half in range(half_count):
        span = slice(half * width, (half + 1) * width)
        real, imag = cosine[:, span].copy(), -sine[:, span]
        real_back, imag_back = 2.0 * cosine[span], -2.0 * sine[span]
        if half == 0:
            imag[:, 0] = cosine[:, extent // 2]
            real_back[0] = 1.0
            imag_back[0] = cosine[extent // 2]
        forward.append(np.concatenate([real, imag], axis=1))
        backward.append(np.concatenate([real_back, imag_back], axis=0))
    col_table = np.concatenate(forward, axis=1)
    lag_table = np.stack(backward)
    row_table = np.concatenate(
        [cosine.reshape(-1, chunk, extent), sine.reshape(-1, chunk, extent)], axis=1
    )
    return tuple(t.astype(jnp.bfloat16) for t in (col_table, row_table, lag_table))


def kernel(
    sizes,
    dest_hbm,
    peaks_hbm,
    sar_hbm,
    opt_hbm,
    col_hbm,
    row_hbm,
    lag_hbm,
    surface_ref,
    peak_ref,
    dest_ref,
    peaks_ref,
    sar_v,
    opt_v,
    col_v,
    row_v,
    lag_v,
    sar_send,
    arrived,
    opt_send,
    opt_cols,
    sar_cols,
    sar_rows,
    cross_send,
    cross_recv,
    cross_own,
    cross_all,
    stat_send,
    stat_recv,
    last_send,
    last_recv,
    lags,
    lag_recv,
    load_sem,
    sar_ssem,
    sar_rsem,
    opt_ssem,
    opt_rsem,
    pair_ssem,
    pair_rsem,
):
    tiles, halves, bands, patch_dev, quarter, extent, lines, chunk, peak_count = sizes
    group = tiles * halves
    width = extent // 2 // halves
    chunks = extent // chunk
    per_half = chunks // halves
    tile, half, band = lax.axis_index("tile"), lax.axis_index("half"), lax.axis_index("band")
    me = tile * halves + half
    other_half = 1 - half
    other_band = 1 - band

    loads = [
        pltpu.make_async_copy(a, b, load_sem.at[i])
        for i, (a, b) in enumerate(
            [(sar_hbm, sar_v), (col_hbm, col_v), (opt_hbm, opt_v), (row_hbm, row_v), (lag_hbm, lag_v),
             (dest_hbm, dest_ref), (peaks_hbm, peaks_ref)]
        )
    ]
    for load in loads:
        load.start()

    barrier = pltpu.get_barrier_semaphore()
    for step in range(tiles):
        for shift in range(halves):
            if step or shift:
                pl.semaphore_signal(
                    barrier,
                    inc=1,
                    device_id={
                        "tile": lax.rem(tile + step, tiles),
                        "half": lax.rem(half + shift, halves),
                    },
                    device_id_type=MESH,
                )
    pl.semaphore_signal(barrier, inc=1, device_id={"band": other_band}, device_id_type=MESH)

    loads[5].wait()
    own_runs = [lax.div(dest_ref[me * group + j], group) for j in range(group)]

    def block_for(run):
        found = jnp.int32(0)
        for j in range(group):
            found = jnp.where(own_runs[j] == run, j, found)
        return found

    def sar_copy(step, shift):
        to_half = lax.rem(half + shift, halves)
        return pltpu.make_async_remote_copy(
            src_ref=sar_send.at[step, to_half],
            dst_ref=arrived.at[me],
            send_sem=sar_ssem.at[step * halves + shift],
            recv_sem=sar_rsem.at[me],
            device_id={"tile": lax.rem(tile + step, tiles), "half": to_half},
            device_id_type=MESH,
        )

    loads[0].wait()
    loads[1].wait()
    order = sorted(range(tiles), key=lambda s: -min(s, tiles - s))
    for step in order:
        to_tile = lax.rem(tile + step, tiles)
        samples = jnp.concatenate(
            [sar_v[block_for(to_tile * halves + run)] for run in range(halves)], axis=0
        )
        spectra = jnp.dot(samples, col_v[...], preferred_element_type=jnp.float32)
        spectra = spectra.astype(jnp.bfloat16)
        for to_half in range(halves):
            piece = spectra[:, to_half * 2 * width : (to_half + 1) * 2 * width]
            sar_send[step, to_half] = piece.reshape(halves, lines, 2 * width)
    arrived[me] = sar_send[0, half]

    rows = pl.ds(pl.multiple_of(half * quarter, quarter), quarter)
    loads[2].wait()
    for turn, patch in enumerate((other_band, band)):
        spectra = jnp.dot(opt_v[patch], col_v[...], preferred_element_type=jnp.float32)
        spectra = spectra.astype(jnp.bfloat16)
        for to_half in range(halves):
            opt_send[turn, to_half] = spectra[:, to_half * 2 * width : (to_half + 1) * 2 * width]
        opt_cols[turn, rows, :] = opt_send[turn, half]

    pl.semaphore_wait(barrier, group)
    copies = []
    for step in order:
        for shift in reversed(range(halves)):
            if step or shift:
                copy = sar_copy(step, shift)
                copy.start()
                copies.append(copy)
    opt_copies = []
    for turn in range(2):
        copy = pltpu.make_async_remote_copy(
            src_ref=opt_send.at[turn, other_half],
            dst_ref=opt_cols.at[turn, rows],
            send_sem=opt_ssem.at[turn],
            recv_sem=opt_rsem.at[turn],
            device_id={"half": other_half},
            device_id_type=MESH,
        )
        copy.start()
        opt_copies.append(copy)

    slot_of = []
    for run in range(halves):
        places = []
        for source in range(group):
            place = jnp.int32(0)
            for j in range(group):
                spot = dest_ref[source * group + j]
                place = jnp.where(
                    lax.div(spot, group) == tile * halves + run, lax.rem(spot, group), place
                )
            places.append(place)
        for slot in range(group):
            found = jnp.int32(0)
            for source in range(group):
                found = jnp.where(places[source] == slot, source, found)
            slot_of.append(found)

    for step in order:
        for shift in range(halves):
            if step or shift:
                source = lax.rem(tile + step, tiles) * halves + lax.rem(half + shift, halves)
                pltpu.make_async_remote_copy(
                    src_ref=sar_send.at[0, 0],
                    dst_ref=arrived.at[source],
                    send_sem=sar_ssem.at[0],
                    recv_sem=sar_rsem.at[source],
                    device_id={"half": other_half},
                    device_id_type=MESH,
                ).wait_recv()
    per_patch = group // patch_dev
    for run in range(halves):
        for slot in range(group):
            at = run * quarter + (slot % per_patch) * lines
            sar_cols[slot // per_patch, at : at + lines, :] = arrived[slot_of[run * group + slot], run]

    loads[3].wait()
    for patch in range(patch_dev):
        for c in range(chunks):
            sar_rows[patch, c] = jnp.dot(
                row_v[c], sar_cols[patch], preferred_element_type=jnp.float32
            )

    lane = lax.broadcasted_iota(jnp.int32, (chunk, width), 1)
    line = lax.broadcasted_iota(jnp.int32, (chunk, width), 0)
    shared = (lane + half) == 0
    centre = (lane + line + half) == 0

    def parts(table_rows, first):
        a, c = table_rows[:chunk, :width], table_rows[:chunk, width:]
        b, d = table_rows[chunk:, :width], table_rows[chunk:, width:]
        if first:
            a = jnp.where(centre, 0.0, a)
        return a, b, c, d

    def cross_chunk(turn, patch, c):
        oa, ob, oc, od = parts(
            jnp.dot(row_v[c], opt_cols[turn], preferred_element_type=jnp.float32), c == 0
        )
        sa, sb, sc, sd = parts(sar_rows[patch, c], c == 0)
        o_re, o_im, s_re, s_im = oa + od, oc - ob, sa + sd, sc - sb
        real = o_re * s_re + o_im * s_im
        imag = o_re * s_im - o_im * s_re
        shared_real = oa * sa + ob * sb - (od * sc - oc * sd)
        shared_imag = ob * sa - oa * sb + (oc * sc + od * sd)
        real = jnp.where(shared, shared_real, real)
        imag = jnp.where(shared, shared_imag, imag)
        o_energy = jnp.sum(o_re * o_re + o_im * o_im, axis=0, keepdims=True)
        s_energy = jnp.sum(s_re * s_re + s_im * s_im, axis=0, keepdims=True)
        return real, imag, o_energy, s_energy

    weight = jnp.where(shared[:1], 1.0, 2.0)

    def pair_copy(k, src, dst, axis, to):
        return pltpu.make_async_remote_copy(
            src_ref=src,
            dst_ref=dst,
            send_sem=pair_ssem.at[k],
            recv_sem=pair_rsem.at[k],
            device_id={axis: to},
            device_id_type=MESH,
        )

    opt_copies[0].wait_recv()
    o_sum, s_sum = 0.0, 0.0
    for c in range(chunks):
        real, imag, o_energy, s_energy = cross_chunk(0, other_band, c)
        cross_send[c, :, :width] = real.astype(jnp.bfloat16)
        cross_send[c, :, width:] = imag.astype(jnp.bfloat16)
        o_sum, s_sum = o_sum + o_energy, s_sum + s_energy
    stat_send[0:1, :] = o_sum * weight
    stat_send[1:2, :] = s_sum * weight
    stat_send[2:8, :] = jnp.zeros((6, width), jnp.float32)
    cross_copy = pair_copy(0, cross_send, cross_recv, "band", other_band)
    cross_copy.start()
    stat_copy = pair_copy(1, stat_send, stat_recv, "band", other_band)
    stat_copy.start()

    opt_copies[1].wait_recv()
    o_sum, s_sum = 0.0, 0.0
    for c in range(chunks):
        real, imag, o_energy, s_energy = cross_chunk(1, band, c)
        cross_own[c, :, :width] = real
        cross_own[c, :, width:] = imag
        o_sum, s_sum = o_sum + o_energy, s_sum + s_energy

    cross_copy.wait_recv()
    for c in range(chunks):
        total = cross_own[c] + cross_recv[c].astype(jnp.float32)
        cross_all[c * chunk : (c + 1) * chunk, :] = total.astype(jnp.bfloat16)

    loads[4].wait()

    def lag_chunk(c):
        both = jnp.dot(row_v[c], cross_all[...], preferred_element_type=jnp.float32)
        lags[c, :, :width] = (both[:chunk, :width] - both[chunk:, width:]).astype(jnp.bfloat16)
        lags[c, :, width:] = (both[:chunk, width:] + both[chunk:, :width]).astype(jnp.bfloat16)

    for i in range(per_half):
        lag_chunk(other_half * per_half + i)
    lag_copy = pair_copy(2, lags.at[pl.ds(other_half * per_half, per_half)], lag_recv, "half", other_half)
    lag_copy.start()
    for i in range(per_half):
        lag_chunk(half * per_half + i)

    spots = lax.broadcasted_iota(jnp.int32, (peak_count, extent), 1)
    ranks = lax.broadcasted_iota(jnp.int32, (peak_count, extent), 0)

    loads[6].wait()

    def one_hot(which):
        wanted = jnp.zeros((peak_count, extent), jnp.int32)
        for j in range(peak_count):
            wanted = jnp.where(ranks == j, peaks_ref[0, which, j], wanted)
        return jnp.where(spots == wanted, 1.0, 0.0).astype(jnp.bfloat16)

    picked = jnp.dot(
        one_hot(0), lags[...].reshape(extent, 2 * width), preferred_element_type=jnp.float32
    )
    waves = lax.dot_general(
        one_hot(1), lag_v[half], (((1,), (1,)), ((), ())), preferred_element_type=jnp.float32
    )
    stat_copy.wait_recv()
    last_send[0:8, :] = stat_recv[...]
    last_send[0:1, :] = o_sum * weight + stat_recv[0:1, :]
    last_send[1:2, :] = s_sum * weight + stat_recv[1:2, :]
    last_send[8 : 8 + peak_count, :] = jnp.broadcast_to(
        jnp.sum(picked * waves, axis=1, keepdims=True), (peak_count, width)
    )
    last_copy = pair_copy(3, last_send, last_recv, "half", other_half)
    last_copy.start()

    own_lags = lags[pl.ds(half * per_half, per_half)].reshape(quarter, 2 * width)
    surface_ref[0] = jnp.dot(own_lags, lag_v[half], preferred_element_type=jnp.float32)

    last_copy.wait_recv()
    totals = last_send[...] + last_recv[...]
    pixels = extent * extent
    o_all = jnp.sum(totals[0:1, :], axis=1, keepdims=True) / (float(pixels) * bands * pixels)
    s_all = jnp.sum(totals[1:2, :], axis=1, keepdims=True) / (float(pixels) * bands * pixels)
    norm = lax.rsqrt(bands * pixels * (o_all + EPSILON) * (s_all + EPSILON)) / pixels
    peak_ref[...] = totals[8 : 8 + peak_count, :] * norm

    lag_copy.wait_recv()
    far = jnp.dot(
        lag_recv[...].reshape(quarter, 2 * width),
        lag_v[other_half],
        preferred_element_type=jnp.float32,
    )
    surface_ref[0] = (surface_ref[0] + far) * norm

    for copy in copies + opt_copies + [cross_copy, stat_copy, lag_copy, last_copy]:
        copy.wait_send()


def fused(mesh, optical, sar, destination, peaks):
    tiles, halves, bands = mesh.shape["tile"], mesh.shape["half"], mesh.shape["band"]
    patch_dev, _, quarter, extent = optical.shape
    group = tiles * halves
    lines = sar.shape[1] // group
    peak_count = peaks.shape[2]
    chunk = quarter // 2
    chunks = extent // chunk
    width = extent // 2 // halves
    sizes = (tiles, halves, bands, patch_dev, quarter, extent, lines, chunk, peak_count)
    tables = half_tables(extent, halves, chunk)
    bf, f32 = jnp.bfloat16, jnp.float32
    wide = 2 * width
    vmem = pltpu.VMEM
    dma = pltpu.SemaphoreType.DMA
    surface, peak_rows = pl.pallas_call(
        functools.partial(kernel, sizes),
        out_shape=(
            jax.ShapeDtypeStruct((1, quarter, extent), f32),
            jax.ShapeDtypeStruct((peak_count, width), f32),
        ),
        in_specs=[pl.BlockSpec(memory_space=pltpu.HBM)] * 7,
        out_specs=(pl.BlockSpec(memory_space=pltpu.VMEM), pl.BlockSpec(memory_space=pltpu.VMEM)),
        scratch_shapes=[
            pltpu.SMEM(destination.shape, jnp.int32),
            pltpu.SMEM(peaks.shape, jnp.int32),
            vmem((group, lines, extent), bf),
            vmem((patch_dev, quarter, extent), bf),
            vmem((extent, extent), bf),
            vmem((chunks, 2 * chunk, extent), bf),
            vmem((halves, wide, extent), bf),
            vmem((tiles, halves, halves, lines, wide), bf),
            vmem((group, halves, lines, wide), bf),
            vmem((patch_dev, halves, quarter, wide), bf),
            vmem((patch_dev, extent, wide), bf),
            vmem((patch_dev, extent, wide), bf),
            vmem((patch_dev, chunks, 2 * chunk, wide), f32),
            vmem((chunks, chunk, wide), bf),
            vmem((chunks, chunk, wide), bf),
            vmem((chunks, chunk, wide), f32),
            vmem((extent, wide), bf),
            vmem((8, width), f32),
            vmem((8, width), f32),
            vmem((8 + peak_count, width), f32),
            vmem((8 + peak_count, width), f32),
            vmem((chunks, chunk, wide), bf),
            vmem((chunks // halves, chunk, wide), bf),
            dma((7,)),
            dma((group,)),
            dma((group,)),
            dma((2,)),
            dma((2,)),
            dma((4,)),
            dma((4,)),
        ],
        compiler_params=pltpu.CompilerParams(
            collective_id=0, has_side_effects=True, vmem_limit_bytes=50 * 1024 * 1024
        ),
    )(
        *[
            pltpu.with_memory_space_constraint(x, pltpu.HBM)
            for x in (
                destination,
                peaks,
                sar.reshape(group, lines, extent),
                optical.reshape(patch_dev, quarter, extent),
                *[jnp.asarray(t) for t in tables],
            )
        ]
    )
    return surface, peak_rows[:, 0].reshape(1, peak_count)


def fits(mesh, optical, sar, peaks):
    group = mesh.shape["tile"] * mesh.shape["half"]
    patch_dev, local_bands, quarter, extent = optical.shape
    lines = sar.shape[1] // group
    return (
        mesh.shape["half"] == 2
        and mesh.shape["band"] == 2
        and patch_dev == 2
        and local_bands == 1
        and lines % 16 == 0
        and quarter % lines == 0
        and extent % 512 == 0
        and peaks.shape[0] == 1
        and peaks.shape[2] % 8 == 0
    )


def solution(mesh):
    def local(optical, sar, destination, peaks):
        if fits(mesh, optical, sar, peaks):
            return fused(mesh, optical, sar, destination, peaks)
        return generic(optical, sar, destination, peaks)

    in_specs = (
        P(("scene", "tile"), "band", "half", None),
        P("band", ("scene", "tile", "half"), None),
        P("scene"),
        P(("scene", "tile", "band"), None, None),
    )
    out_specs = (P(("scene", "tile", "band"), "half", None), P(("scene", "tile", "band"), None))
    return jax.shard_map(local, mesh=mesh, in_specs=in_specs, out_specs=out_specs, check_vma=False)
```

```python
import functools
import math

import jax
import jax.numpy as jnp
import numpy as np
from jax import lax
from jax.experimental import pallas as pl
from jax.experimental.pallas import tpu as pltpu
from jax.sharding import PartitionSpec as P

MESH = pl.DeviceIdType.MESH

precise = lax.Precision.HIGHEST
EPSILON = 1e-06


def fourier_tables(extent):
    places = jnp.arange(extent, dtype=jnp.int32)
    phases = places[:, None] * places[None, :] % extent
    angles = phases.astype(jnp.float32) * (2.0 * math.pi / extent)
    return (jnp.cos(angles), jnp.sin(angles))


def fourier_pair(table):
    upper = table.astype(jnp.bfloat16)
    lower = (table - upper.astype(jnp.float32)).astype(jnp.bfloat16)
    return (upper, lower)


def column_spectrum(samples, table_upper, table_lower):
    extent = samples.shape[-1]
    values = samples.reshape(-1, extent)
    spectrum = jnp.dot(values, table_upper, preferred_element_type=jnp.float32) + jnp.dot(
        values, table_lower, preferred_element_type=jnp.float32
    )
    return spectrum.astype(jnp.bfloat16).reshape(samples.shape[:-1] + (2 * extent,))


def row_spectrum(columns, table_upper, table_lower):
    line_count = columns.shape[-3]
    stacked = jnp.concatenate([columns[..., 0, :], columns[..., 1, :]], axis=-2)
    result = jnp.einsum("kr,...rc->...kc", table_upper, stacked, preferred_element_type=jnp.float32)
    result = result + jnp.einsum(
        "kr,...rc->...kc", table_lower, stacked, preferred_element_type=jnp.float32
    )
    return (result[..., :line_count, :], result[..., line_count:, :])


def relay_blocks(parcel):
    layout = parcel.shape
    merged = parcel.reshape(layout[:1] + (layout[1] * layout[2],) + layout[3:])
    arrived = lax.all_to_all(merged, ("tile", "half"), split_axis=1, concat_axis=1, tiled=True)
    return arrived.reshape(layout)


def generic(optical, sar, destination, peaks):
    tile_count = lax.axis_size("tile")
    half_count = lax.axis_size("half")
    band_count = lax.axis_size("band")
    group_size = tile_count * half_count
    patch_dev, local_bands, quarter, extent = optical.shape
    col_width = extent // half_count
    block_lines = sar.shape[1] // group_size
    band_total = local_bands * band_count
    pixel_count = extent * extent
    patch_total = patch_dev * tile_count
    kept_patches = patch_dev // band_count
    cosine_table, sine_table = fourier_tables(extent)
    col_upper, col_lower = fourier_pair(jnp.concatenate([cosine_table, -sine_table], axis=1))
    row_full = jnp.concatenate(
        [
            jnp.concatenate([cosine_table, sine_table], axis=1),
            jnp.concatenate([-sine_table, cosine_table], axis=1),
        ],
        axis=0,
    )
    row_upper, row_lower = fourier_pair(row_full)
    tile_at = lax.axis_index("tile")
    half_at = lax.axis_index("half")
    band_at = lax.axis_index("band")
    device_at = lax.axis_index(("tile", "half"))
    own_blocks = lax.dynamic_slice_in_dim(destination, device_at * group_size, group_size)
    send_order = jnp.argsort(own_blocks // group_size)
    inverse = (
        jnp.zeros_like(destination)
        .at[destination]
        .set(jnp.arange(destination.shape[0], dtype=jnp.int32))
    )
    opt_values = optical.astype(jnp.float32)
    opt_sums = jnp.sum(opt_values, axis=(2, 3))
    opt_squares = jnp.sum(opt_values * opt_values, axis=(2, 3))
    sar_values = sar.astype(jnp.float32).reshape(local_bands, group_size, block_lines * extent)
    sar_sums = jnp.sum(sar_values, axis=2)
    sar_squares = jnp.sum(sar_values * sar_values, axis=2)
    map_device = own_blocks // group_size
    map_patch = (
        map_device // half_count * patch_dev + own_blocks % group_size * block_lines // quarter
    )
    member = (map_patch[:, None] == jnp.arange(patch_total, dtype=jnp.int32)[None, :]).astype(
        jnp.float32
    )
    sar_stats = jnp.dot(
        jnp.stack([sar_sums, sar_squares]).reshape(2 * local_bands, group_size),
        member,
        precision=precise,
        preferred_element_type=jnp.float32,
    )
    statistics = jnp.zeros((2, 2, band_total, patch_total), jnp.float32)
    opt_part = jnp.transpose(jnp.stack([opt_sums, opt_squares]), (0, 2, 1))
    statistics = lax.dynamic_update_slice(
        statistics, opt_part[None], (0, 0, band_at * local_bands, tile_at * patch_dev)
    )
    statistics = lax.dynamic_update_slice(
        statistics,
        sar_stats.reshape(2, local_bands, patch_total)[None],
        (1, 0, band_at * local_bands, 0),
    )
    totals = lax.psum(statistics, ("tile", "half", "band"))
    centered = totals[:, 1] - totals[:, 0] * totals[:, 0] / pixel_count
    energy = jnp.sum(centered, axis=1) / (band_total * pixel_count)
    norm_scale = lax.rsqrt(band_total * pixel_count * (energy[0] + EPSILON) * (energy[1] + EPSILON))
    first_patch = tile_at * patch_dev + band_at * kept_patches
    norm_mine = lax.dynamic_slice_in_dim(norm_scale, first_patch, kept_patches)
    slant_spectra = column_spectrum(sar, col_upper, col_lower).reshape(
        local_bands, group_size, block_lines, 2, half_count, col_width
    )
    outgoing = jnp.take(slant_spectra, send_order, axis=1).reshape(
        local_bands, tile_count, half_count, block_lines, 2, half_count, col_width
    )
    outgoing = jnp.transpose(outgoing, (0, 1, 5, 2, 3, 4, 6))
    arrived = relay_blocks(outgoing).reshape(
        local_bands, group_size * half_count, block_lines, 2, col_width
    )
    sources = lax.dynamic_slice_in_dim(
        inverse, tile_at * half_count * group_size, half_count * group_size
    )
    slot_index = (
        sources // group_size * half_count
        + jnp.arange(half_count * group_size, dtype=jnp.int32) // group_size
    )
    placed = jnp.take(arrived, slot_index, axis=1).reshape(
        local_bands, half_count, patch_dev, quarter, 2, col_width
    )
    placed = jnp.transpose(placed, (2, 0, 1, 3, 4, 5)).reshape(
        patch_dev, local_bands, extent, 2, col_width
    )
    sar_real, sar_imag = row_spectrum(placed, row_upper, row_lower)
    spectra = column_spectrum(optical, col_upper, col_lower).reshape(
        patch_dev, local_bands, quarter, 2, half_count, col_width
    )
    real_part, imag_part = row_spectrum(
        jnp.squeeze(
            lax.all_to_all(spectra, "half", split_axis=4, concat_axis=2, tiled=True), axis=4
        ),
        row_upper,
        row_lower,
    )
    opt_real = real_part
    opt_imag = imag_part
    rows_at = jnp.arange(extent, dtype=jnp.int32)[:, None]
    cols_at = half_at * col_width + jnp.arange(col_width, dtype=jnp.int32)[None, :]
    keep_mask = jnp.where((rows_at == 0) & (cols_at == 0), 0.0, 1.0).astype(jnp.float32)
    opt_real = opt_real * keep_mask
    opt_imag = opt_imag * keep_mask
    sar_real = sar_real * keep_mask
    sar_imag = sar_imag * keep_mask
    cross_real = jnp.sum(opt_real * sar_real + opt_imag * sar_imag, axis=1)
    cross_imag = jnp.sum(opt_real * sar_imag - opt_imag * sar_real, axis=1)
    cross_term = jnp.stack([cross_real, cross_imag], axis=1)
    cross_sum = lax.psum_scatter(cross_term, "band", scatter_dimension=0, tiled=True)
    lag_real = (
        jnp.einsum("uk,pkc->puc", cosine_table, cross_sum[:, 0], precision=precise)
        - jnp.einsum("uk,pkc->puc", sine_table, cross_sum[:, 1], precision=precise)
    ) / extent
    lag_imag = (
        jnp.einsum("uk,pkc->puc", cosine_table, cross_sum[:, 1], precision=precise)
        + jnp.einsum("uk,pkc->puc", sine_table, cross_sum[:, 0], precision=precise)
    ) / extent
    lagged = jnp.stack([lag_real, lag_imag], axis=2).reshape(
        kept_patches, half_count, quarter, 2, col_width
    )
    pieces = lax.all_to_all(lagged, "half", split_axis=1, concat_axis=4, tiled=True)
    real_in = pieces[:, 0, :, 0, :]
    imag_in = pieces[:, 0, :, 1, :]
    correlation = (
        jnp.einsum("puc,cv->puv", real_in, cosine_table, precision=precise)
        - jnp.einsum("puc,cv->puv", imag_in, sine_table, precision=precise)
    ) / extent
    surface = correlation * norm_mine[:, None, None]
    local_rows = peaks[:, 0, :] - half_at * quarter
    row_hit = (
        local_rows[:, :, None] == jnp.arange(quarter, dtype=jnp.int32)[None, None, :]
    ).astype(jnp.float32)
    picked = jnp.einsum("pkr,prc->pkc", row_hit, surface, precision=precise)
    col_hit = (peaks[:, 1, :, None] == jnp.arange(extent, dtype=jnp.int32)[None, None, :]).astype(
        jnp.float32
    )
    local_values = jnp.sum(picked * col_hit, axis=2)
    peak_values = lax.psum(local_values, "half")
    return (surface, peak_values)


def half_tables(extent, half_count, chunk):
    width = extent // 2 // half_count
    places = np.arange(extent)
    phases = (places[:, None] * places[None, :]) % extent
    cosine = np.cos(phases * (2.0 * np.pi / extent))
    sine = np.sin(phases * (2.0 * np.pi / extent))
    forward, backward = [], []
    for half in range(half_count):
        span = slice(half * width, (half + 1) * width)
        real, imag = cosine[:, span].copy(), -sine[:, span]
        real_back, imag_back = 2.0 * cosine[span], -2.0 * sine[span]
        if half == 0:
            imag[:, 0] = cosine[:, extent // 2]
            real_back[0] = 1.0
            imag_back[0] = cosine[extent // 2]
        forward.append(np.concatenate([real, imag], axis=1))
        backward.append(np.concatenate([real_back, imag_back], axis=0))
    col_table = np.concatenate(forward, axis=1)
    lag_table = np.stack(backward)
    row_table = np.concatenate(
        [cosine.reshape(-1, chunk, extent), sine.reshape(-1, chunk, extent)], axis=1
    )
    return tuple(t.astype(jnp.bfloat16) for t in (col_table, row_table, lag_table))


def kernel(
    sizes,
    dest_hbm,
    peaks_hbm,
    sar_hbm,
    opt_hbm,
    col_hbm,
    row_hbm,
    lag_hbm,
    surface_ref,
    total_ref,
    dest_ref,
    peaks_ref,
    sar_v,
    opt_v,
    col_v,
    row_v,
    lag_v,
    sar_send,
    arrived,
    opt_send,
    opt_cols,
    sar_cols,
    sar_rows,
    cross_send,
    cross_recv,
    cross_own,
    cross_all,
    stat_send,
    stat_recv,
    last_send,
    last_recv,
    lags,
    lag_recv,
    load_sem,
    sar_ssem,
    sar_rsem,
    opt_ssem,
    opt_rsem,
    pair_ssem,
    pair_rsem,
):
    tiles, halves, bands, patch_dev, quarter, extent, lines, chunk, peak_count = sizes
    group = tiles * halves
    width = extent // 2 // halves
    chunks = extent // chunk
    per_half = chunks // halves
    tile, half, band = lax.axis_index("tile"), lax.axis_index("half"), lax.axis_index("band")
    me = tile * halves + half
    other_half = 1 - half
    other_band = 1 - band

    loads = [
        pltpu.make_async_copy(a, b, load_sem.at[i])
        for i, (a, b) in enumerate(
            [(sar_hbm, sar_v), (col_hbm, col_v), (opt_hbm, opt_v), (row_hbm, row_v), (lag_hbm, lag_v),
             (dest_hbm, dest_ref), (peaks_hbm, peaks_ref)]
        )
    ]
    for i in (5, 0, 1, 2):
        loads[i].start()

    barrier = pltpu.get_barrier_semaphore()
    for step in range(tiles):
        for shift in range(halves):
            if step or shift:
                pl.semaphore_signal(
                    barrier,
                    inc=1,
                    device_id={
                        "tile": lax.rem(tile + step, tiles),
                        "half": lax.rem(half + shift, halves),
                    },
                    device_id_type=MESH,
                )
    pl.semaphore_signal(barrier, inc=1, device_id={"band": other_band}, device_id_type=MESH)

    loads[5].wait()
    own_runs = [lax.div(dest_ref[me * group + j], group) for j in range(group)]

    def block_for(run):
        found = jnp.int32(0)
        for j in range(group):
            found = jnp.where(own_runs[j] == run, j, found)
        return found

    def sar_copy(step, shift):
        to_half = lax.rem(half + shift, halves)
        return pltpu.make_async_remote_copy(
            src_ref=sar_send.at[step, to_half],
            dst_ref=arrived.at[me],
            send_sem=sar_ssem.at[step * halves + shift],
            recv_sem=sar_rsem.at[me],
            device_id={"tile": lax.rem(tile + step, tiles), "half": to_half},
            device_id_type=MESH,
        )

    loads[0].wait()
    loads[1].wait()
    copies = []
    opt_copies = []
    order = sorted(range(tiles), key=lambda s: -min(s, tiles - s))
    for turn, step in enumerate(order):
        to_tile = lax.rem(tile + step, tiles)
        samples = jnp.concatenate(
            [sar_v[block_for(to_tile * halves + run)] for run in range(halves)], axis=0
        )
        spectra = jnp.dot(samples, col_v[...], preferred_element_type=jnp.float32)
        spectra = spectra.astype(jnp.bfloat16)
        for to_half in range(halves):
            piece = spectra[:, to_half * 2 * width : (to_half + 1) * 2 * width]
            sar_send[step, to_half] = piece.reshape(halves, lines, 2 * width)
        if turn == 0:
            for i in (3, 4, 6):
                loads[i].start()
        if turn == 1:
            pl.semaphore_wait(barrier, group)
        for ready in order[:2] if turn == 1 else (order[turn : turn + 1] if turn > 1 else ()):
            for shift in reversed(range(halves)):
                if ready or shift:
                    copy = sar_copy(ready, shift)
                    copy.start()
                    copies.append(copy)
    arrived[me] = sar_send[0, half]

    rows = pl.ds(pl.multiple_of(half * quarter, quarter), quarter)
    loads[2].wait()
    for turn, patch in enumerate((other_band, band)):
        spectra = jnp.dot(opt_v[patch], col_v[...], preferred_element_type=jnp.float32)
        spectra = spectra.astype(jnp.bfloat16)
        for to_half in range(halves):
            opt_send[turn, to_half] = spectra[:, to_half * 2 * width : (to_half + 1) * 2 * width]
        copy = pltpu.make_async_remote_copy(
            src_ref=opt_send.at[turn, other_half],
            dst_ref=opt_cols.at[turn, rows],
            send_sem=opt_ssem.at[turn],
            recv_sem=opt_rsem.at[turn],
            device_id={"half": other_half},
            device_id_type=MESH,
        )
        copy.start()
        opt_copies.append(copy)
        opt_cols[turn, rows, :] = opt_send[turn, half]

    slot_of = []
    for run in range(halves):
        places = []
        for source in range(group):
            place = jnp.int32(0)
            for j in range(group):
                spot = dest_ref[source * group + j]
                place = jnp.where(
                    lax.div(spot, group) == tile * halves + run, lax.rem(spot, group), place
                )
            places.append(place)
        for slot in range(group):
            found = jnp.int32(0)
            for source in range(group):
                found = jnp.where(places[source] == slot, source, found)
            slot_of.append(found)

    for step in order:
        for shift in range(halves):
            if step or shift:
                source = lax.rem(tile + step, tiles) * halves + lax.rem(half + shift, halves)
                pltpu.make_async_remote_copy(
                    src_ref=sar_send.at[0, 0],
                    dst_ref=arrived.at[source],
                    send_sem=sar_ssem.at[0],
                    recv_sem=sar_rsem.at[source],
                    device_id={"half": other_half},
                    device_id_type=MESH,
                ).wait_recv()
    per_patch = group // patch_dev
    for run in range(halves):
        for slot in range(group):
            at = run * quarter + (slot % per_patch) * lines
            sar_cols[slot // per_patch, at : at + lines, :] = arrived[slot_of[run * group + slot], run]

    loads[3].wait()
    for patch in range(patch_dev):
        for c in range(chunks):
            sar_rows[patch, c] = jnp.dot(
                row_v[c], sar_cols[patch], preferred_element_type=jnp.float32
            )

    lane = lax.broadcasted_iota(jnp.int32, (chunk, width), 1)
    line = lax.broadcasted_iota(jnp.int32, (chunk, width), 0)
    shared = (lane + half) == 0
    centre = (lane + line + half) == 0

    def parts(table_rows, first):
        a, c = table_rows[:chunk, :width], table_rows[:chunk, width:]
        b, d = table_rows[chunk:, :width], table_rows[chunk:, width:]
        if first:
            a = jnp.where(centre, 0.0, a)
        return a, b, c, d

    def cross_chunk(turn, patch, c):
        oa, ob, oc, od = parts(
            jnp.dot(row_v[c], opt_cols[turn], preferred_element_type=jnp.float32), c == 0
        )
        sa, sb, sc, sd = parts(sar_rows[patch, c], c == 0)
        o_re, o_im, s_re, s_im = oa + od, oc - ob, sa + sd, sc - sb
        real = o_re * s_re + o_im * s_im
        imag = o_re * s_im - o_im * s_re
        shared_real = oa * sa + ob * sb - (od * sc - oc * sd)
        shared_imag = ob * sa - oa * sb + (oc * sc + od * sd)
        real = jnp.where(shared, shared_real, real)
        imag = jnp.where(shared, shared_imag, imag)
        o_energy = jnp.sum(o_re * o_re + o_im * o_im, axis=0, keepdims=True)
        s_energy = jnp.sum(s_re * s_re + s_im * s_im, axis=0, keepdims=True)
        return real, imag, o_energy, s_energy

    weight = jnp.where(shared[:1], 1.0, 2.0)

    def pair_copy(k, src, dst, axis, to):
        return pltpu.make_async_remote_copy(
            src_ref=src,
            dst_ref=dst,
            send_sem=pair_ssem.at[k],
            recv_sem=pair_rsem.at[k],
            device_id={axis: to},
            device_id_type=MESH,
        )

    opt_copies[0].wait_recv()
    o_sum, s_sum = 0.0, 0.0
    for c in range(chunks):
        real, imag, o_energy, s_energy = cross_chunk(0, other_band, c)
        cross_send[c, :, :width] = real.astype(jnp.bfloat16)
        cross_send[c, :, width:] = imag.astype(jnp.bfloat16)
        o_sum, s_sum = o_sum + o_energy, s_sum + s_energy
    stat_send[0:1, :] = o_sum * weight
    stat_send[1:2, :] = s_sum * weight
    stat_send[2:8, :] = jnp.zeros((6, width), jnp.float32)
    cross_copy = pair_copy(0, cross_send, cross_recv, "band", other_band)
    cross_copy.start()
    stat_copy = pair_copy(1, stat_send, stat_recv, "band", other_band)
    stat_copy.start()

    opt_copies[1].wait_recv()
    o_sum, s_sum = 0.0, 0.0
    for c in range(chunks):
        real, imag, o_energy, s_energy = cross_chunk(1, band, c)
        cross_own[c, :, :width] = real
        cross_own[c, :, width:] = imag
        o_sum, s_sum = o_sum + o_energy, s_sum + s_energy

    cross_copy.wait_recv()
    for c in range(chunks):
        total = cross_own[c] + cross_recv[c].astype(jnp.float32)
        cross_all[c * chunk : (c + 1) * chunk, :] = total.astype(jnp.bfloat16)

    loads[4].wait()

    def lag_chunk(c):
        both = jnp.dot(row_v[c], cross_all[...], preferred_element_type=jnp.float32)
        lags[c, :, :width] = (both[:chunk, :width] - both[chunk:, width:]).astype(jnp.bfloat16)
        lags[c, :, width:] = (both[:chunk, width:] + both[chunk:, :width]).astype(jnp.bfloat16)

    lag_copies = []
    for i in range(per_half):
        at = other_half * per_half + i
        lag_chunk(at)
        copy = pair_copy(3 + i, lags.at[at], lag_recv.at[i], "half", other_half)
        copy.start()
        lag_copies.append(copy)
    for i in range(per_half):
        lag_chunk(half * per_half + i)

    spots = lax.broadcasted_iota(jnp.int32, (peak_count, extent), 1)
    ranks = lax.broadcasted_iota(jnp.int32, (peak_count, extent), 0)

    loads[6].wait()

    def one_hot(which):
        wanted = jnp.zeros((peak_count, extent), jnp.int32)
        for j in range(peak_count):
            wanted = jnp.where(ranks == j, peaks_ref[0, which, j], wanted)
        return jnp.where(spots == wanted, 1.0, 0.0).astype(jnp.bfloat16)

    picked = jnp.dot(
        one_hot(0), lags[...].reshape(extent, 2 * width), preferred_element_type=jnp.float32
    )
    waves = lax.dot_general(
        one_hot(1), lag_v[half], (((1,), (1,)), ((), ())), preferred_element_type=jnp.float32
    )
    stat_copy.wait_recv()
    last_send[0:8, :] = stat_recv[...]
    last_send[0:1, :] = o_sum * weight + stat_recv[0:1, :]
    last_send[1:2, :] = s_sum * weight + stat_recv[1:2, :]
    last_send[8 : 8 + peak_count, :] = jnp.broadcast_to(
        jnp.sum(picked * waves, axis=1, keepdims=True), (peak_count, width)
    )
    last_copy = pair_copy(2, last_send, last_recv, "half", other_half)
    last_copy.start()

    for i in range(per_half):
        at = slice(i * chunk, (i + 1) * chunk)
        near = lags[half * per_half + i]
        surface_ref[0, at, :] = jnp.dot(near, lag_v[half], preferred_element_type=jnp.float32)

    for i in range(per_half):
        at = slice(i * chunk, (i + 1) * chunk)
        lag_copies[i].wait_recv()
        far = jnp.dot(lag_recv[i], lag_v[other_half], preferred_element_type=jnp.float32)
        surface_ref[0, at, :] = surface_ref[0, at, :] + far

    last_copy.wait_recv()
    total_ref[...] = last_send[...] + last_recv[...]
    for copy in copies + opt_copies + lag_copies + [cross_copy, stat_copy, last_copy]:
        copy.wait_send()


def finish(bands, pieces, surface_ref, total_ref, out_ref, peak_ref, scaled, sem):
    _, lines, extent = surface_ref.shape
    pixels = extent * extent
    peak_count = peak_ref.shape[1]
    width = total_ref.shape[1]
    o_all = jnp.sum(total_ref[0:1, :], axis=1, keepdims=True) / (float(pixels) * bands * pixels)
    s_all = jnp.sum(total_ref[1:2, :], axis=1, keepdims=True) / (float(pixels) * bands * pixels)
    norm = lax.rsqrt(bands * pixels * (o_all + EPSILON) * (s_all + EPSILON)) / pixels
    part = lines // pieces
    copies = []
    for i in range(pieces):
        at = pl.ds(i * part, part)
        scaled[at, :] = surface_ref[0, at, :] * norm
        copy = pltpu.make_async_copy(scaled.at[at], out_ref.at[0, at], sem.at[i])
        copy.start()
        copies.append(copy)
    values = total_ref[8 : 8 + peak_count, :] * norm
    lane = lax.broadcasted_iota(jnp.int32, (peak_count, width), 1)
    rank = lax.broadcasted_iota(jnp.int32, (peak_count, width), 0)
    row = jnp.sum(jnp.where(lane == rank, values, 0.0), axis=0, keepdims=True)
    peak_ref[...] = row[:, :peak_count]
    for copy in copies:
        copy.wait()


def fused(mesh, optical, sar, destination, peaks):
    tiles, halves, bands = mesh.shape["tile"], mesh.shape["half"], mesh.shape["band"]
    patch_dev, _, quarter, extent = optical.shape
    group = tiles * halves
    lines = sar.shape[1] // group
    peak_count = peaks.shape[2]
    chunk = quarter // 2
    chunks = extent // chunk
    width = extent // 2 // halves
    sizes = (tiles, halves, bands, patch_dev, quarter, extent, lines, chunk, peak_count)
    tables = half_tables(extent, halves, chunk)
    bf, f32 = jnp.bfloat16, jnp.float32
    wide = 2 * width
    vmem = pltpu.VMEM
    dma = pltpu.SemaphoreType.DMA
    raw, totals = pl.pallas_call(
        functools.partial(kernel, sizes),
        out_shape=(
            jax.ShapeDtypeStruct((1, quarter, extent), f32),
            jax.ShapeDtypeStruct((8 + peak_count, width), f32),
        ),
        in_specs=[pl.BlockSpec(memory_space=pltpu.HBM)] * 7,
        out_specs=(pl.BlockSpec(memory_space=pltpu.VMEM), pl.BlockSpec(memory_space=pltpu.VMEM)),
        scratch_shapes=[
            pltpu.SMEM(destination.shape, jnp.int32),
            pltpu.SMEM(peaks.shape, jnp.int32),
            vmem((group, lines, extent), bf),
            vmem((patch_dev, quarter, extent), bf),
            vmem((extent, extent), bf),
            vmem((chunks, 2 * chunk, extent), bf),
            vmem((halves, wide, extent), bf),
            vmem((tiles, halves, halves, lines, wide), bf),
            vmem((group, halves, lines, wide), bf),
            vmem((patch_dev, halves, quarter, wide), bf),
            vmem((patch_dev, extent, wide), bf),
            vmem((patch_dev, extent, wide), bf),
            vmem((patch_dev, chunks, 2 * chunk, wide), f32),
            vmem((chunks, chunk, wide), bf),
            vmem((chunks, chunk, wide), bf),
            vmem((chunks, chunk, wide), f32),
            vmem((extent, wide), bf),
            vmem((8, width), f32),
            vmem((8, width), f32),
            vmem((8 + peak_count, width), f32),
            vmem((8 + peak_count, width), f32),
            vmem((chunks, chunk, wide), bf),
            vmem((chunks // halves, chunk, wide), bf),
            dma((7,)),
            dma((group,)),
            dma((group,)),
            dma((2,)),
            dma((2,)),
            dma((3 + chunks // halves,)),
            dma((3 + chunks // halves,)),
        ],
        compiler_params=pltpu.CompilerParams(
            collective_id=0, has_side_effects=True, vmem_limit_bytes=50 * 1024 * 1024
        ),
    )(
        *[
            pltpu.with_memory_space_constraint(x, pltpu.HBM)
            for x in (
                destination,
                peaks,
                sar.reshape(group, lines, extent),
                optical.reshape(patch_dev, quarter, extent),
                *[jnp.asarray(t) for t in tables],
            )
        ]
    )
    pieces = 4
    return pl.pallas_call(
        functools.partial(finish, bands, pieces),
        out_shape=(
            jax.ShapeDtypeStruct((1, quarter, extent), f32),
            jax.ShapeDtypeStruct((1, peak_count), f32),
        ),
        in_specs=[pl.BlockSpec(memory_space=pltpu.VMEM)] * 2,
        out_specs=(pl.BlockSpec(memory_space=pltpu.HBM), pl.BlockSpec(memory_space=pltpu.VMEM)),
        scratch_shapes=[vmem((quarter, extent), f32), dma((pieces,))],
    )(*[pltpu.with_memory_space_constraint(x, pltpu.VMEM) for x in (raw, totals)])


def fits(mesh, optical, sar, peaks):
    group = mesh.shape["tile"] * mesh.shape["half"]
    patch_dev, local_bands, quarter, extent = optical.shape
    lines = sar.shape[1] // group
    return (
        mesh.shape["half"] == 2
        and mesh.shape["band"] == 2
        and patch_dev == 2
        and local_bands == 1
        and lines % 16 == 0
        and quarter % lines == 0
        and extent % 512 == 0
        and peaks.shape[0] == 1
        and peaks.shape[2] % 8 == 0
    )


def solution(mesh):
    def local(optical, sar, destination, peaks):
        if fits(mesh, optical, sar, peaks):
            return fused(mesh, optical, sar, destination, peaks)
        return generic(optical, sar, destination, peaks)

    in_specs = (
        P(("scene", "tile"), "band", "half", None),
        P("band", ("scene", "tile", "half"), None),
        P("scene"),
        P(("scene", "tile", "band"), None, None),
    )
    out_specs = (P(("scene", "tile", "band"), "half", None), P(("scene", "tile", "band"), None))
    return jax.shard_map(local, mesh=mesh, in_specs=in_specs, out_specs=out_specs, check_vma=False)
```

```python
import functools
import math

import jax
import jax.numpy as jnp
import numpy as np
from jax import lax
from jax.experimental import pallas as pl
from jax.experimental.pallas import tpu as pltpu
from jax.sharding import PartitionSpec as P

MESH = pl.DeviceIdType.MESH

precise = lax.Precision.HIGHEST
EPSILON = 1e-06


def fourier_tables(extent):
    places = jnp.arange(extent, dtype=jnp.int32)
    phases = places[:, None] * places[None, :] % extent
    angles = phases.astype(jnp.float32) * (2.0 * math.pi / extent)
    return (jnp.cos(angles), jnp.sin(angles))


def fourier_pair(table):
    upper = table.astype(jnp.bfloat16)
    lower = (table - upper.astype(jnp.float32)).astype(jnp.bfloat16)
    return (upper, lower)


def column_spectrum(samples, table_upper, table_lower):
    extent = samples.shape[-1]
    values = samples.reshape(-1, extent)
    spectrum = jnp.dot(values, table_upper, preferred_element_type=jnp.float32) + jnp.dot(
        values, table_lower, preferred_element_type=jnp.float32
    )
    return spectrum.astype(jnp.bfloat16).reshape(samples.shape[:-1] + (2 * extent,))


def row_spectrum(columns, table_upper, table_lower):
    line_count = columns.shape[-3]
    stacked = jnp.concatenate([columns[..., 0, :], columns[..., 1, :]], axis=-2)
    result = jnp.einsum("kr,...rc->...kc", table_upper, stacked, preferred_element_type=jnp.float32)
    result = result + jnp.einsum(
        "kr,...rc->...kc", table_lower, stacked, preferred_element_type=jnp.float32
    )
    return (result[..., :line_count, :], result[..., line_count:, :])


def relay_blocks(parcel):
    layout = parcel.shape
    merged = parcel.reshape(layout[:1] + (layout[1] * layout[2],) + layout[3:])
    arrived = lax.all_to_all(merged, ("tile", "half"), split_axis=1, concat_axis=1, tiled=True)
    return arrived.reshape(layout)


def generic(optical, sar, destination, peaks):
    tile_count = lax.axis_size("tile")
    half_count = lax.axis_size("half")
    band_count = lax.axis_size("band")
    group_size = tile_count * half_count
    patch_dev, local_bands, quarter, extent = optical.shape
    col_width = extent // half_count
    block_lines = sar.shape[1] // group_size
    band_total = local_bands * band_count
    pixel_count = extent * extent
    patch_total = patch_dev * tile_count
    kept_patches = patch_dev // band_count
    cosine_table, sine_table = fourier_tables(extent)
    col_upper, col_lower = fourier_pair(jnp.concatenate([cosine_table, -sine_table], axis=1))
    row_full = jnp.concatenate(
        [
            jnp.concatenate([cosine_table, sine_table], axis=1),
            jnp.concatenate([-sine_table, cosine_table], axis=1),
        ],
        axis=0,
    )
    row_upper, row_lower = fourier_pair(row_full)
    tile_at = lax.axis_index("tile")
    half_at = lax.axis_index("half")
    band_at = lax.axis_index("band")
    device_at = lax.axis_index(("tile", "half"))
    own_blocks = lax.dynamic_slice_in_dim(destination, device_at * group_size, group_size)
    send_order = jnp.argsort(own_blocks // group_size)
    inverse = (
        jnp.zeros_like(destination)
        .at[destination]
        .set(jnp.arange(destination.shape[0], dtype=jnp.int32))
    )
    opt_values = optical.astype(jnp.float32)
    opt_sums = jnp.sum(opt_values, axis=(2, 3))
    opt_squares = jnp.sum(opt_values * opt_values, axis=(2, 3))
    sar_values = sar.astype(jnp.float32).reshape(local_bands, group_size, block_lines * extent)
    sar_sums = jnp.sum(sar_values, axis=2)
    sar_squares = jnp.sum(sar_values * sar_values, axis=2)
    map_device = own_blocks // group_size
    map_patch = (
        map_device // half_count * patch_dev + own_blocks % group_size * block_lines // quarter
    )
    member = (map_patch[:, None] == jnp.arange(patch_total, dtype=jnp.int32)[None, :]).astype(
        jnp.float32
    )
    sar_stats = jnp.dot(
        jnp.stack([sar_sums, sar_squares]).reshape(2 * local_bands, group_size),
        member,
        precision=precise,
        preferred_element_type=jnp.float32,
    )
    statistics = jnp.zeros((2, 2, band_total, patch_total), jnp.float32)
    opt_part = jnp.transpose(jnp.stack([opt_sums, opt_squares]), (0, 2, 1))
    statistics = lax.dynamic_update_slice(
        statistics, opt_part[None], (0, 0, band_at * local_bands, tile_at * patch_dev)
    )
    statistics = lax.dynamic_update_slice(
        statistics,
        sar_stats.reshape(2, local_bands, patch_total)[None],
        (1, 0, band_at * local_bands, 0),
    )
    totals = lax.psum(statistics, ("tile", "half", "band"))
    centered = totals[:, 1] - totals[:, 0] * totals[:, 0] / pixel_count
    energy = jnp.sum(centered, axis=1) / (band_total * pixel_count)
    norm_scale = lax.rsqrt(band_total * pixel_count * (energy[0] + EPSILON) * (energy[1] + EPSILON))
    first_patch = tile_at * patch_dev + band_at * kept_patches
    norm_mine = lax.dynamic_slice_in_dim(norm_scale, first_patch, kept_patches)
    slant_spectra = column_spectrum(sar, col_upper, col_lower).reshape(
        local_bands, group_size, block_lines, 2, half_count, col_width
    )
    outgoing = jnp.take(slant_spectra, send_order, axis=1).reshape(
        local_bands, tile_count, half_count, block_lines, 2, half_count, col_width
    )
    outgoing = jnp.transpose(outgoing, (0, 1, 5, 2, 3, 4, 6))
    arrived = relay_blocks(outgoing).reshape(
        local_bands, group_size * half_count, block_lines, 2, col_width
    )
    sources = lax.dynamic_slice_in_dim(
        inverse, tile_at * half_count * group_size, half_count * group_size
    )
    slot_index = (
        sources // group_size * half_count
        + jnp.arange(half_count * group_size, dtype=jnp.int32) // group_size
    )
    placed = jnp.take(arrived, slot_index, axis=1).reshape(
        local_bands, half_count, patch_dev, quarter, 2, col_width
    )
    placed = jnp.transpose(placed, (2, 0, 1, 3, 4, 5)).reshape(
        patch_dev, local_bands, extent, 2, col_width
    )
    sar_real, sar_imag = row_spectrum(placed, row_upper, row_lower)
    spectra = column_spectrum(optical, col_upper, col_lower).reshape(
        patch_dev, local_bands, quarter, 2, half_count, col_width
    )
    real_part, imag_part = row_spectrum(
        jnp.squeeze(
            lax.all_to_all(spectra, "half", split_axis=4, concat_axis=2, tiled=True), axis=4
        ),
        row_upper,
        row_lower,
    )
    opt_real = real_part
    opt_imag = imag_part
    rows_at = jnp.arange(extent, dtype=jnp.int32)[:, None]
    cols_at = half_at * col_width + jnp.arange(col_width, dtype=jnp.int32)[None, :]
    keep_mask = jnp.where((rows_at == 0) & (cols_at == 0), 0.0, 1.0).astype(jnp.float32)
    opt_real = opt_real * keep_mask
    opt_imag = opt_imag * keep_mask
    sar_real = sar_real * keep_mask
    sar_imag = sar_imag * keep_mask
    cross_real = jnp.sum(opt_real * sar_real + opt_imag * sar_imag, axis=1)
    cross_imag = jnp.sum(opt_real * sar_imag - opt_imag * sar_real, axis=1)
    cross_term = jnp.stack([cross_real, cross_imag], axis=1)
    cross_sum = lax.psum_scatter(cross_term, "band", scatter_dimension=0, tiled=True)
    lag_real = (
        jnp.einsum("uk,pkc->puc", cosine_table, cross_sum[:, 0], precision=precise)
        - jnp.einsum("uk,pkc->puc", sine_table, cross_sum[:, 1], precision=precise)
    ) / extent
    lag_imag = (
        jnp.einsum("uk,pkc->puc", cosine_table, cross_sum[:, 1], precision=precise)
        + jnp.einsum("uk,pkc->puc", sine_table, cross_sum[:, 0], precision=precise)
    ) / extent
    lagged = jnp.stack([lag_real, lag_imag], axis=2).reshape(
        kept_patches, half_count, quarter, 2, col_width
    )
    pieces = lax.all_to_all(lagged, "half", split_axis=1, concat_axis=4, tiled=True)
    real_in = pieces[:, 0, :, 0, :]
    imag_in = pieces[:, 0, :, 1, :]
    correlation = (
        jnp.einsum("puc,cv->puv", real_in, cosine_table, precision=precise)
        - jnp.einsum("puc,cv->puv", imag_in, sine_table, precision=precise)
    ) / extent
    surface = correlation * norm_mine[:, None, None]
    local_rows = peaks[:, 0, :] - half_at * quarter
    row_hit = (
        local_rows[:, :, None] == jnp.arange(quarter, dtype=jnp.int32)[None, None, :]
    ).astype(jnp.float32)
    picked = jnp.einsum("pkr,prc->pkc", row_hit, surface, precision=precise)
    col_hit = (peaks[:, 1, :, None] == jnp.arange(extent, dtype=jnp.int32)[None, None, :]).astype(
        jnp.float32
    )
    local_values = jnp.sum(picked * col_hit, axis=2)
    peak_values = lax.psum(local_values, "half")
    return (surface, peak_values)


def half_tables(extent, half_count, chunk):
    width = extent // 2 // half_count
    places = np.arange(extent)
    phases = (places[:, None] * places[None, :]) % extent
    cosine = np.cos(phases * (2.0 * np.pi / extent))
    sine = np.sin(phases * (2.0 * np.pi / extent))
    forward, backward = [], []
    for half in range(half_count):
        span = slice(half * width, (half + 1) * width)
        real, imag = cosine[:, span].copy(), -sine[:, span]
        real_back, imag_back = 2.0 * cosine[span], -2.0 * sine[span]
        if half == 0:
            imag[:, 0] = cosine[:, extent // 2]
            real_back[0] = 1.0
            imag_back[0] = cosine[extent // 2]
        forward.append(np.concatenate([real, imag], axis=1))
        backward.append(np.concatenate([real_back, imag_back], axis=0))
    col_table = np.concatenate(forward, axis=1)
    lag_table = np.stack(backward)
    row_table = np.concatenate(
        [cosine.reshape(-1, chunk, extent), sine.reshape(-1, chunk, extent)], axis=1
    )
    return tuple(t.astype(jnp.bfloat16) for t in (col_table, row_table, lag_table))


def kernel(
    sizes,
    dest_hbm,
    peaks_hbm,
    sar_hbm,
    opt_hbm,
    col_hbm,
    row_hbm,
    lag_hbm,
    surface_ref,
    total_ref,
    dest_ref,
    peaks_ref,
    sar_v,
    opt_v,
    col_v,
    row_v,
    lag_v,
    sar_send,
    arrived,
    opt_send,
    opt_far,
    opt_near,
    sar_cols,
    sar_rows,
    cross_send,
    cross_recv,
    cross_all,
    stat_send,
    stat_recv,
    last_send,
    last_recv,
    lags,
    lag_recv,
    load_sem,
    sar_ssem,
    sar_rsem,
    opt_ssem,
    opt_rsem,
    pair_ssem,
    pair_rsem,
):
    tiles, halves, bands, patch_dev, quarter, extent, lines, chunk, peak_count = sizes
    group = tiles * halves
    width = extent // 2 // halves
    chunks = extent // chunk
    per_half = chunks // halves
    tile, half, band = lax.axis_index("tile"), lax.axis_index("half"), lax.axis_index("band")
    me = tile * halves + half
    other_half = 1 - half
    other_band = 1 - band

    loads = [
        pltpu.make_async_copy(a, b, load_sem.at[i])
        for i, (a, b) in enumerate(
            [(sar_hbm, sar_v), (col_hbm, col_v), (opt_hbm, opt_v), (row_hbm, row_v), (lag_hbm, lag_v),
             (dest_hbm, dest_ref), (peaks_hbm, peaks_ref)]
        )
    ]
    for i in (5, 0, 1, 2):
        loads[i].start()

    barrier = pltpu.get_barrier_semaphore()
    for step in range(tiles):
        for shift in range(halves):
            if step or shift:
                pl.semaphore_signal(
                    barrier,
                    inc=1,
                    device_id={
                        "tile": lax.rem(tile + step, tiles),
                        "half": lax.rem(half + shift, halves),
                    },
                    device_id_type=MESH,
                )
    pl.semaphore_signal(barrier, inc=1, device_id={"band": other_band}, device_id_type=MESH)

    loads[5].wait()
    own_runs = [lax.div(dest_ref[me * group + j], group) for j in range(group)]

    def block_for(run):
        found = jnp.int32(0)
        for j in range(group):
            found = jnp.where(own_runs[j] == run, j, found)
        return found

    def sar_copy(step, shift):
        to_half = lax.rem(half + shift, halves)
        return pltpu.make_async_remote_copy(
            src_ref=sar_send.at[step, to_half],
            dst_ref=arrived.at[me],
            send_sem=sar_ssem.at[step * halves + shift],
            recv_sem=sar_rsem.at[me],
            device_id={"tile": lax.rem(tile + step, tiles), "half": to_half},
            device_id_type=MESH,
        )

    loads[0].wait()
    loads[1].wait()
    copies = []
    opt_copies = []
    order = sorted(range(tiles), key=lambda s: -min(s, tiles - s))
    for turn, step in enumerate(order):
        to_tile = lax.rem(tile + step, tiles)
        samples = jnp.concatenate(
            [sar_v[block_for(to_tile * halves + run)] for run in range(halves)], axis=0
        )
        spectra = jnp.dot(samples, col_v[...], preferred_element_type=jnp.float32)
        spectra = spectra.astype(jnp.bfloat16)
        for to_half in range(halves):
            piece = spectra[:, to_half * 2 * width : (to_half + 1) * 2 * width]
            sar_send[step, to_half] = piece.reshape(halves, lines, 2 * width)
        if turn == 0:
            for i in (3, 4, 6):
                loads[i].start()
        if turn == 1:
            pl.semaphore_wait(barrier, group)
        for ready in order[:2] if turn == 1 else (order[turn : turn + 1] if turn > 1 else ()):
            for shift in reversed(range(halves)):
                if ready or shift:
                    copy = sar_copy(ready, shift)
                    copy.start()
                    copies.append(copy)
    arrived[me] = sar_send[0, half]

    loads[2].wait()
    for turn, patch in enumerate((other_band, band)):
        spectra = jnp.dot(opt_v[patch], col_v[...], preferred_element_type=jnp.float32)
        spectra = spectra.astype(jnp.bfloat16)
        for to_half in range(halves):
            opt_send[turn, to_half] = spectra[:, to_half * 2 * width : (to_half + 1) * 2 * width]
        copy = pltpu.make_async_remote_copy(
            src_ref=opt_send.at[turn, other_half],
            dst_ref=opt_far.at[turn],
            send_sem=opt_ssem.at[turn],
            recv_sem=opt_rsem.at[turn],
            device_id={"half": other_half},
            device_id_type=MESH,
        )
        copy.start()
        opt_copies.append(copy)

    slot_of = []
    for run in range(halves):
        places = []
        for source in range(group):
            place = jnp.int32(0)
            for j in range(group):
                spot = dest_ref[source * group + j]
                place = jnp.where(
                    lax.div(spot, group) == tile * halves + run, lax.rem(spot, group), place
                )
            places.append(place)
        for slot in range(group):
            found = jnp.int32(0)
            for source in range(group):
                found = jnp.where(places[source] == slot, source, found)
            slot_of.append(found)

    near_lines = pl.ds(pl.multiple_of(half * quarter, quarter), quarter)
    far_lines = pl.ds(pl.multiple_of(other_half * quarter, quarter), quarter)
    loads[3].wait()
    for turn in range(2):
        for c in range(chunks):
            opt_near[turn, c] = jnp.dot(
                row_v[c, :, near_lines], opt_send[turn, half], preferred_element_type=jnp.float32
            )

    for step in order:
        for shift in range(halves):
            if step or shift:
                source = lax.rem(tile + step, tiles) * halves + lax.rem(half + shift, halves)
                pltpu.make_async_remote_copy(
                    src_ref=sar_send.at[0, 0],
                    dst_ref=arrived.at[source],
                    send_sem=sar_ssem.at[0],
                    recv_sem=sar_rsem.at[source],
                    device_id={"half": other_half},
                    device_id_type=MESH,
                ).wait_recv()
    per_patch = group // patch_dev
    for run in range(halves):
        for slot in range(group):
            at = run * quarter + (slot % per_patch) * lines
            sar_cols[slot // per_patch, at : at + lines, :] = arrived[slot_of[run * group + slot], run]

    for patch in range(patch_dev):
        for c in range(chunks):
            sar_rows[patch, c] = jnp.dot(
                row_v[c], sar_cols[patch], preferred_element_type=jnp.float32
            )

    lane = lax.broadcasted_iota(jnp.int32, (chunk, width), 1)
    line = lax.broadcasted_iota(jnp.int32, (chunk, width), 0)
    shared = (lane + half) == 0
    centre = (lane + line + half) == 0

    def parts(table_rows, first):
        a, c = table_rows[:chunk, :width], table_rows[:chunk, width:]
        b, d = table_rows[chunk:, :width], table_rows[chunk:, width:]
        if first:
            a = jnp.where(centre, 0.0, a)
        return a, b, c, d

    def cross_chunk(turn, patch, c):
        far = jnp.dot(
            row_v[c, :, far_lines], opt_far[turn], preferred_element_type=jnp.float32
        )
        oa, ob, oc, od = parts(opt_near[turn, c] + far, c == 0)
        sa, sb, sc, sd = parts(sar_rows[patch, c], c == 0)
        o_re, o_im, s_re, s_im = oa + od, oc - ob, sa + sd, sc - sb
        real = o_re * s_re + o_im * s_im
        imag = o_re * s_im - o_im * s_re
        shared_real = oa * sa + ob * sb - (od * sc - oc * sd)
        shared_imag = ob * sa - oa * sb + (oc * sc + od * sd)
        real = jnp.where(shared, shared_real, real)
        imag = jnp.where(shared, shared_imag, imag)
        o_energy = jnp.sum(o_re * o_re + o_im * o_im, axis=0, keepdims=True)
        s_energy = jnp.sum(s_re * s_re + s_im * s_im, axis=0, keepdims=True)
        return real, imag, o_energy, s_energy

    weight = jnp.where(shared[:1], 1.0, 2.0)

    def pair_copy(k, src, dst, axis, to):
        return pltpu.make_async_remote_copy(
            src_ref=src,
            dst_ref=dst,
            send_sem=pair_ssem.at[k],
            recv_sem=pair_rsem.at[k],
            device_id={axis: to},
            device_id_type=MESH,
        )

    opt_copies[0].wait_recv()
    o_sum, s_sum = 0.0, 0.0
    for c in range(chunks):
        real, imag, o_energy, s_energy = cross_chunk(0, other_band, c)
        cross_send[c, :, :width] = real.astype(jnp.bfloat16)
        cross_send[c, :, width:] = imag.astype(jnp.bfloat16)
        o_sum, s_sum = o_sum + o_energy, s_sum + s_energy
    stat_send[0:1, :] = o_sum * weight
    stat_send[1:2, :] = s_sum * weight
    stat_send[2:8, :] = jnp.zeros((6, width), jnp.float32)
    cross_copy = pair_copy(0, cross_send, cross_recv, "band", other_band)
    cross_copy.start()
    stat_copy = pair_copy(1, stat_send, stat_recv, "band", other_band)
    stat_copy.start()

    opt_copies[1].wait_recv()
    cross_copy.wait_recv()
    o_sum, s_sum = 0.0, 0.0
    for c in range(chunks):
        real, imag, o_energy, s_energy = cross_chunk(1, band, c)
        at = slice(c * chunk, (c + 1) * chunk)
        real = real + cross_recv[c, :, :width].astype(jnp.float32)
        imag = imag + cross_recv[c, :, width:].astype(jnp.float32)
        cross_all[at, :width] = real.astype(jnp.bfloat16)
        cross_all[at, width:] = imag.astype(jnp.bfloat16)
        o_sum, s_sum = o_sum + o_energy, s_sum + s_energy

    loads[4].wait()

    def lag_chunk(c):
        both = jnp.dot(row_v[c], cross_all[...], preferred_element_type=jnp.float32)
        lags[c, :, :width] = (both[:chunk, :width] - both[chunk:, width:]).astype(jnp.bfloat16)
        lags[c, :, width:] = (both[:chunk, width:] + both[chunk:, :width]).astype(jnp.bfloat16)

    lag_copies = []
    for i in range(per_half):
        at = other_half * per_half + i
        lag_chunk(at)
        copy = pair_copy(3 + i, lags.at[at], lag_recv.at[i], "half", other_half)
        copy.start()
        lag_copies.append(copy)
    for i in range(per_half):
        lag_chunk(half * per_half + i)

    spots = lax.broadcasted_iota(jnp.int32, (peak_count, extent), 1)
    ranks = lax.broadcasted_iota(jnp.int32, (peak_count, extent), 0)

    loads[6].wait()

    def one_hot(which):
        wanted = jnp.zeros((peak_count, extent), jnp.int32)
        for j in range(peak_count):
            wanted = jnp.where(ranks == j, peaks_ref[0, which, j], wanted)
        return jnp.where(spots == wanted, 1.0, 0.0).astype(jnp.bfloat16)

    picked = jnp.dot(
        one_hot(0), lags[...].reshape(extent, 2 * width), preferred_element_type=jnp.float32
    )
    waves = lax.dot_general(
        one_hot(1), lag_v[half], (((1,), (1,)), ((), ())), preferred_element_type=jnp.float32
    )
    stat_copy.wait_recv()
    last_send[0:8, :] = stat_recv[...]
    last_send[0:1, :] = o_sum * weight + stat_recv[0:1, :]
    last_send[1:2, :] = s_sum * weight + stat_recv[1:2, :]
    last_send[8 : 8 + peak_count, :] = jnp.broadcast_to(
        jnp.sum(picked * waves, axis=1, keepdims=True), (peak_count, width)
    )
    last_copy = pair_copy(2, last_send, last_recv, "half", other_half)
    last_copy.start()

    for i in range(per_half):
        at = slice(i * chunk, (i + 1) * chunk)
        near = lags[half * per_half + i]
        surface_ref[0, at, :] = jnp.dot(near, lag_v[half], preferred_element_type=jnp.float32)

    for i in range(per_half):
        at = slice(i * chunk, (i + 1) * chunk)
        lag_copies[i].wait_recv()
        far = jnp.dot(lag_recv[i], lag_v[other_half], preferred_element_type=jnp.float32)
        surface_ref[0, at, :] = surface_ref[0, at, :] + far

    last_copy.wait_recv()
    total_ref[...] = last_send[...] + last_recv[...]
    for copy in copies + opt_copies + lag_copies + [cross_copy, stat_copy, last_copy]:
        copy.wait_send()


def finish(bands, pieces, surface_ref, total_ref, out_ref, peak_ref, scaled, sem):
    _, lines, extent = surface_ref.shape
    pixels = extent * extent
    peak_count = peak_ref.shape[1]
    width = total_ref.shape[1]
    o_all = jnp.sum(total_ref[0:1, :], axis=1, keepdims=True) / (float(pixels) * bands * pixels)
    s_all = jnp.sum(total_ref[1:2, :], axis=1, keepdims=True) / (float(pixels) * bands * pixels)
    norm = lax.rsqrt(bands * pixels * (o_all + EPSILON) * (s_all + EPSILON)) / pixels
    part = lines // pieces
    copies = []
    for i in range(pieces):
        at = pl.ds(i * part, part)
        scaled[at, :] = surface_ref[0, at, :] * norm
        copy = pltpu.make_async_copy(scaled.at[at], out_ref.at[0, at], sem.at[i])
        copy.start()
        copies.append(copy)
    values = total_ref[8 : 8 + peak_count, :] * norm
    lane = lax.broadcasted_iota(jnp.int32, (peak_count, width), 1)
    rank = lax.broadcasted_iota(jnp.int32, (peak_count, width), 0)
    row = jnp.sum(jnp.where(lane == rank, values, 0.0), axis=0, keepdims=True)
    peak_ref[...] = row[:, :peak_count]
    for copy in copies:
        copy.wait()


def fused(mesh, optical, sar, destination, peaks):
    tiles, halves, bands = mesh.shape["tile"], mesh.shape["half"], mesh.shape["band"]
    patch_dev, _, quarter, extent = optical.shape
    group = tiles * halves
    lines = sar.shape[1] // group
    peak_count = peaks.shape[2]
    chunk = quarter // 2
    chunks = extent // chunk
    width = extent // 2 // halves
    sizes = (tiles, halves, bands, patch_dev, quarter, extent, lines, chunk, peak_count)
    tables = half_tables(extent, halves, chunk)
    bf, f32 = jnp.bfloat16, jnp.float32
    wide = 2 * width
    vmem = pltpu.VMEM
    dma = pltpu.SemaphoreType.DMA
    raw, totals = pl.pallas_call(
        functools.partial(kernel, sizes),
        out_shape=(
            jax.ShapeDtypeStruct((1, quarter, extent), f32),
            jax.ShapeDtypeStruct((8 + peak_count, width), f32),
        ),
        in_specs=[pl.BlockSpec(memory_space=pltpu.HBM)] * 7,
        out_specs=(pl.BlockSpec(memory_space=pltpu.VMEM), pl.BlockSpec(memory_space=pltpu.VMEM)),
        scratch_shapes=[
            pltpu.SMEM(destination.shape, jnp.int32),
            pltpu.SMEM(peaks.shape, jnp.int32),
            vmem((group, lines, extent), bf),
            vmem((patch_dev, quarter, extent), bf),
            vmem((extent, extent), bf),
            vmem((chunks, 2 * chunk, extent), bf),
            vmem((halves, wide, extent), bf),
            vmem((tiles, halves, halves, lines, wide), bf),
            vmem((group, halves, lines, wide), bf),
            vmem((patch_dev, halves, quarter, wide), bf),
            vmem((patch_dev, quarter, wide), bf),
            vmem((patch_dev, chunks, 2 * chunk, wide), f32),
            vmem((patch_dev, extent, wide), bf),
            vmem((patch_dev, chunks, 2 * chunk, wide), f32),
            vmem((chunks, chunk, wide), bf),
            vmem((chunks, chunk, wide), bf),
            vmem((extent, wide), bf),
            vmem((8, width), f32),
            vmem((8, width), f32),
            vmem((8 + peak_count, width), f32),
            vmem((8 + peak_count, width), f32),
            vmem((chunks, chunk, wide), bf),
            vmem((chunks // halves, chunk, wide), bf),
            dma((7,)),
            dma((group,)),
            dma((group,)),
            dma((2,)),
            dma((2,)),
            dma((3 + chunks // halves,)),
            dma((3 + chunks // halves,)),
        ],
        compiler_params=pltpu.CompilerParams(
            collective_id=0, has_side_effects=True, vmem_limit_bytes=50 * 1024 * 1024
        ),
    )(
        *[
            pltpu.with_memory_space_constraint(x, pltpu.HBM)
            for x in (
                destination,
                peaks,
                sar.reshape(group, lines, extent),
                optical.reshape(patch_dev, quarter, extent),
                *[jnp.asarray(t) for t in tables],
            )
        ]
    )
    pieces = 4
    return pl.pallas_call(
        functools.partial(finish, bands, pieces),
        out_shape=(
            jax.ShapeDtypeStruct((1, quarter, extent), f32),
            jax.ShapeDtypeStruct((1, peak_count), f32),
        ),
        in_specs=[pl.BlockSpec(memory_space=pltpu.VMEM)] * 2,
        out_specs=(pl.BlockSpec(memory_space=pltpu.HBM), pl.BlockSpec(memory_space=pltpu.VMEM)),
        scratch_shapes=[vmem((quarter, extent), f32), dma((pieces,))],
    )(*[pltpu.with_memory_space_constraint(x, pltpu.VMEM) for x in (raw, totals)])


def fits(mesh, optical, sar, peaks):
    group = mesh.shape["tile"] * mesh.shape["half"]
    patch_dev, local_bands, quarter, extent = optical.shape
    lines = sar.shape[1] // group
    return (
        mesh.shape["half"] == 2
        and mesh.shape["band"] == 2
        and patch_dev == 2
        and local_bands == 1
        and lines % 16 == 0
        and quarter % lines == 0
        and extent % 512 == 0
        and peaks.shape[0] == 1
        and peaks.shape[2] % 8 == 0
    )


def solution(mesh):
    def local(optical, sar, destination, peaks):
        if fits(mesh, optical, sar, peaks):
            return fused(mesh, optical, sar, destination, peaks)
        return generic(optical, sar, destination, peaks)

    in_specs = (
        P(("scene", "tile"), "band", "half", None),
        P("band", ("scene", "tile", "half"), None),
        P("scene"),
        P(("scene", "tile", "band"), None, None),
    )
    out_specs = (P(("scene", "tile", "band"), "half", None), P(("scene", "tile", "band"), None))
    return jax.shard_map(local, mesh=mesh, in_specs=in_specs, out_specs=out_specs, check_vma=False)
```

```python
import functools
import math

import jax
import jax.numpy as jnp
import numpy as np
from jax import lax
from jax.experimental import pallas as pl
from jax.experimental.pallas import tpu as pltpu
from jax.sharding import PartitionSpec as P

MESH = pl.DeviceIdType.MESH

precise = lax.Precision.HIGHEST
EPSILON = 1e-06


def fourier_tables(extent):
    places = jnp.arange(extent, dtype=jnp.int32)
    phases = places[:, None] * places[None, :] % extent
    angles = phases.astype(jnp.float32) * (2.0 * math.pi / extent)
    return (jnp.cos(angles), jnp.sin(angles))


def fourier_pair(table):
    upper = table.astype(jnp.bfloat16)
    lower = (table - upper.astype(jnp.float32)).astype(jnp.bfloat16)
    return (upper, lower)


def column_spectrum(samples, table_upper, table_lower):
    extent = samples.shape[-1]
    values = samples.reshape(-1, extent)
    spectrum = jnp.dot(values, table_upper, preferred_element_type=jnp.float32) + jnp.dot(
        values, table_lower, preferred_element_type=jnp.float32
    )
    return spectrum.astype(jnp.bfloat16).reshape(samples.shape[:-1] + (2 * extent,))


def row_spectrum(columns, table_upper, table_lower):
    line_count = columns.shape[-3]
    stacked = jnp.concatenate([columns[..., 0, :], columns[..., 1, :]], axis=-2)
    result = jnp.einsum("kr,...rc->...kc", table_upper, stacked, preferred_element_type=jnp.float32)
    result = result + jnp.einsum(
        "kr,...rc->...kc", table_lower, stacked, preferred_element_type=jnp.float32
    )
    return (result[..., :line_count, :], result[..., line_count:, :])


def relay_blocks(parcel):
    layout = parcel.shape
    merged = parcel.reshape(layout[:1] + (layout[1] * layout[2],) + layout[3:])
    arrived = lax.all_to_all(merged, ("tile", "half"), split_axis=1, concat_axis=1, tiled=True)
    return arrived.reshape(layout)


def generic(optical, sar, destination, peaks):
    tile_count = lax.axis_size("tile")
    half_count = lax.axis_size("half")
    band_count = lax.axis_size("band")
    group_size = tile_count * half_count
    patch_dev, local_bands, quarter, extent = optical.shape
    col_width = extent // half_count
    block_lines = sar.shape[1] // group_size
    band_total = local_bands * band_count
    pixel_count = extent * extent
    patch_total = patch_dev * tile_count
    kept_patches = patch_dev // band_count
    cosine_table, sine_table = fourier_tables(extent)
    col_upper, col_lower = fourier_pair(jnp.concatenate([cosine_table, -sine_table], axis=1))
    row_full = jnp.concatenate(
        [
            jnp.concatenate([cosine_table, sine_table], axis=1),
            jnp.concatenate([-sine_table, cosine_table], axis=1),
        ],
        axis=0,
    )
    row_upper, row_lower = fourier_pair(row_full)
    tile_at = lax.axis_index("tile")
    half_at = lax.axis_index("half")
    band_at = lax.axis_index("band")
    device_at = lax.axis_index(("tile", "half"))
    own_blocks = lax.dynamic_slice_in_dim(destination, device_at * group_size, group_size)
    send_order = jnp.argsort(own_blocks // group_size)
    inverse = (
        jnp.zeros_like(destination)
        .at[destination]
        .set(jnp.arange(destination.shape[0], dtype=jnp.int32))
    )
    opt_values = optical.astype(jnp.float32)
    opt_sums = jnp.sum(opt_values, axis=(2, 3))
    opt_squares = jnp.sum(opt_values * opt_values, axis=(2, 3))
    sar_values = sar.astype(jnp.float32).reshape(local_bands, group_size, block_lines * extent)
    sar_sums = jnp.sum(sar_values, axis=2)
    sar_squares = jnp.sum(sar_values * sar_values, axis=2)
    map_device = own_blocks // group_size
    map_patch = (
        map_device // half_count * patch_dev + own_blocks % group_size * block_lines // quarter
    )
    member = (map_patch[:, None] == jnp.arange(patch_total, dtype=jnp.int32)[None, :]).astype(
        jnp.float32
    )
    sar_stats = jnp.dot(
        jnp.stack([sar_sums, sar_squares]).reshape(2 * local_bands, group_size),
        member,
        precision=precise,
        preferred_element_type=jnp.float32,
    )
    statistics = jnp.zeros((2, 2, band_total, patch_total), jnp.float32)
    opt_part = jnp.transpose(jnp.stack([opt_sums, opt_squares]), (0, 2, 1))
    statistics = lax.dynamic_update_slice(
        statistics, opt_part[None], (0, 0, band_at * local_bands, tile_at * patch_dev)
    )
    statistics = lax.dynamic_update_slice(
        statistics,
        sar_stats.reshape(2, local_bands, patch_total)[None],
        (1, 0, band_at * local_bands, 0),
    )
    totals = lax.psum(statistics, ("tile", "half", "band"))
    centered = totals[:, 1] - totals[:, 0] * totals[:, 0] / pixel_count
    energy = jnp.sum(centered, axis=1) / (band_total * pixel_count)
    norm_scale = lax.rsqrt(band_total * pixel_count * (energy[0] + EPSILON) * (energy[1] + EPSILON))
    first_patch = tile_at * patch_dev + band_at * kept_patches
    norm_mine = lax.dynamic_slice_in_dim(norm_scale, first_patch, kept_patches)
    slant_spectra = column_spectrum(sar, col_upper, col_lower).reshape(
        local_bands, group_size, block_lines, 2, half_count, col_width
    )
    outgoing = jnp.take(slant_spectra, send_order, axis=1).reshape(
        local_bands, tile_count, half_count, block_lines, 2, half_count, col_width
    )
    outgoing = jnp.transpose(outgoing, (0, 1, 5, 2, 3, 4, 6))
    arrived = relay_blocks(outgoing).reshape(
        local_bands, group_size * half_count, block_lines, 2, col_width
    )
    sources = lax.dynamic_slice_in_dim(
        inverse, tile_at * half_count * group_size, half_count * group_size
    )
    slot_index = (
        sources // group_size * half_count
        + jnp.arange(half_count * group_size, dtype=jnp.int32) // group_size
    )
    placed = jnp.take(arrived, slot_index, axis=1).reshape(
        local_bands, half_count, patch_dev, quarter, 2, col_width
    )
    placed = jnp.transpose(placed, (2, 0, 1, 3, 4, 5)).reshape(
        patch_dev, local_bands, extent, 2, col_width
    )
    sar_real, sar_imag = row_spectrum(placed, row_upper, row_lower)
    spectra = column_spectrum(optical, col_upper, col_lower).reshape(
        patch_dev, local_bands, quarter, 2, half_count, col_width
    )
    real_part, imag_part = row_spectrum(
        jnp.squeeze(
            lax.all_to_all(spectra, "half", split_axis=4, concat_axis=2, tiled=True), axis=4
        ),
        row_upper,
        row_lower,
    )
    opt_real = real_part
    opt_imag = imag_part
    rows_at = jnp.arange(extent, dtype=jnp.int32)[:, None]
    cols_at = half_at * col_width + jnp.arange(col_width, dtype=jnp.int32)[None, :]
    keep_mask = jnp.where((rows_at == 0) & (cols_at == 0), 0.0, 1.0).astype(jnp.float32)
    opt_real = opt_real * keep_mask
    opt_imag = opt_imag * keep_mask
    sar_real = sar_real * keep_mask
    sar_imag = sar_imag * keep_mask
    cross_real = jnp.sum(opt_real * sar_real + opt_imag * sar_imag, axis=1)
    cross_imag = jnp.sum(opt_real * sar_imag - opt_imag * sar_real, axis=1)
    cross_term = jnp.stack([cross_real, cross_imag], axis=1)
    cross_sum = lax.psum_scatter(cross_term, "band", scatter_dimension=0, tiled=True)
    lag_real = (
        jnp.einsum("uk,pkc->puc", cosine_table, cross_sum[:, 0], precision=precise)
        - jnp.einsum("uk,pkc->puc", sine_table, cross_sum[:, 1], precision=precise)
    ) / extent
    lag_imag = (
        jnp.einsum("uk,pkc->puc", cosine_table, cross_sum[:, 1], precision=precise)
        + jnp.einsum("uk,pkc->puc", sine_table, cross_sum[:, 0], precision=precise)
    ) / extent
    lagged = jnp.stack([lag_real, lag_imag], axis=2).reshape(
        kept_patches, half_count, quarter, 2, col_width
    )
    pieces = lax.all_to_all(lagged, "half", split_axis=1, concat_axis=4, tiled=True)
    real_in = pieces[:, 0, :, 0, :]
    imag_in = pieces[:, 0, :, 1, :]
    correlation = (
        jnp.einsum("puc,cv->puv", real_in, cosine_table, precision=precise)
        - jnp.einsum("puc,cv->puv", imag_in, sine_table, precision=precise)
    ) / extent
    surface = correlation * norm_mine[:, None, None]
    local_rows = peaks[:, 0, :] - half_at * quarter
    row_hit = (
        local_rows[:, :, None] == jnp.arange(quarter, dtype=jnp.int32)[None, None, :]
    ).astype(jnp.float32)
    picked = jnp.einsum("pkr,prc->pkc", row_hit, surface, precision=precise)
    col_hit = (peaks[:, 1, :, None] == jnp.arange(extent, dtype=jnp.int32)[None, None, :]).astype(
        jnp.float32
    )
    local_values = jnp.sum(picked * col_hit, axis=2)
    peak_values = lax.psum(local_values, "half")
    return (surface, peak_values)


def half_tables(extent, half_count, chunk):
    width = extent // 2 // half_count
    places = np.arange(extent)
    phases = (places[:, None] * places[None, :]) % extent
    cosine = np.cos(phases * (2.0 * np.pi / extent))
    sine = np.sin(phases * (2.0 * np.pi / extent))
    forward, backward = [], []
    for half in range(half_count):
        span = slice(half * width, (half + 1) * width)
        real, imag = cosine[:, span].copy(), -sine[:, span]
        real_back, imag_back = 2.0 * cosine[span], -2.0 * sine[span]
        if half == 0:
            imag[:, 0] = cosine[:, extent // 2]
            real_back[0] = 1.0
            imag_back[0] = cosine[extent // 2]
        forward.append(np.concatenate([real, imag], axis=1))
        backward.append(np.concatenate([real_back, imag_back], axis=0))
    col_table = np.concatenate(forward, axis=1)
    lag_table = np.stack(backward)
    row_table = np.concatenate(
        [cosine.reshape(-1, chunk, extent), sine.reshape(-1, chunk, extent)], axis=1
    )
    return tuple(t.astype(jnp.bfloat16) for t in (col_table, row_table, lag_table))


def kernel(
    sizes,
    dest_hbm,
    peaks_hbm,
    sar_hbm,
    opt_hbm,
    col_hbm,
    row_hbm,
    lag_hbm,
    surface_ref,
    total_ref,
    dest_ref,
    peaks_ref,
    sar_v,
    opt_v,
    col_v,
    row_v,
    lag_v,
    sar_send,
    arrived,
    opt_send,
    opt_cols,
    sar_cols,
    sar_rows,
    cross_send,
    cross_recv,
    cross_all,
    stat_send,
    stat_recv,
    last_send,
    last_recv,
    lags,
    lag_recv,
    load_sem,
    sar_ssem,
    sar_rsem,
    opt_ssem,
    opt_rsem,
    pair_ssem,
    pair_rsem,
):
    tiles, halves, bands, patch_dev, quarter, extent, lines, chunk, peak_count = sizes
    group = tiles * halves
    width = extent // 2 // halves
    chunks = extent // chunk
    per_half = chunks // halves
    tile, half, band = lax.axis_index("tile"), lax.axis_index("half"), lax.axis_index("band")
    me = tile * halves + half
    other_half = 1 - half
    other_band = 1 - band

    loads = [
        pltpu.make_async_copy(a, b, load_sem.at[i])
        for i, (a, b) in enumerate(
            [(sar_hbm, sar_v), (col_hbm, col_v), (opt_hbm, opt_v), (row_hbm, row_v), (lag_hbm, lag_v),
             (dest_hbm, dest_ref), (peaks_hbm, peaks_ref)]
        )
    ]
    for i in (5, 0, 1, 2):
        loads[i].start()

    barrier = pltpu.get_barrier_semaphore()
    for step in range(tiles):
        for shift in range(halves):
            if step or shift:
                pl.semaphore_signal(
                    barrier,
                    inc=1,
                    device_id={
                        "tile": lax.rem(tile + step, tiles),
                        "half": lax.rem(half + shift, halves),
                    },
                    device_id_type=MESH,
                )
    pl.semaphore_signal(barrier, inc=1, device_id={"band": other_band}, device_id_type=MESH)

    loads[5].wait()
    own_runs = [lax.div(dest_ref[me * group + j], group) for j in range(group)]

    def block_for(run):
        found = jnp.int32(0)
        for j in range(group):
            found = jnp.where(own_runs[j] == run, j, found)
        return found

    def sar_copy(step, shift):
        to_half = lax.rem(half + shift, halves)
        return pltpu.make_async_remote_copy(
            src_ref=sar_send.at[step, to_half],
            dst_ref=arrived.at[me],
            send_sem=sar_ssem.at[step * halves + shift],
            recv_sem=sar_rsem.at[me],
            device_id={"tile": lax.rem(tile + step, tiles), "half": to_half},
            device_id_type=MESH,
        )

    loads[0].wait()
    loads[1].wait()
    copies = []
    opt_copies = []
    order = sorted(range(tiles), key=lambda s: -min(s, tiles - s))
    for turn, step in enumerate(order):
        to_tile = lax.rem(tile + step, tiles)
        samples = jnp.concatenate(
            [sar_v[block_for(to_tile * halves + run)] for run in range(halves)], axis=0
        )
        spectra = jnp.dot(samples, col_v[...], preferred_element_type=jnp.float32)
        spectra = spectra.astype(jnp.bfloat16)
        for to_half in range(halves):
            piece = spectra[:, to_half * 2 * width : (to_half + 1) * 2 * width]
            sar_send[step, to_half] = piece.reshape(halves, lines, 2 * width)
        if turn == 0:
            for i in (3, 4, 6):
                loads[i].start()
        if turn == 1:
            pl.semaphore_wait(barrier, group)
        for ready in order[:2] if turn == 1 else (order[turn : turn + 1] if turn > 1 else ()):
            for shift in reversed(range(halves)):
                if ready or shift:
                    copy = sar_copy(ready, shift)
                    copy.start()
                    copies.append(copy)
    arrived[me] = sar_send[0, half]

    rows = pl.ds(pl.multiple_of(half * quarter, quarter), quarter)
    loads[2].wait()
    for turn, patch in enumerate((other_band, band)):
        spectra = jnp.dot(opt_v[patch], col_v[...], preferred_element_type=jnp.float32)
        spectra = spectra.astype(jnp.bfloat16)
        for to_half in range(halves):
            opt_send[turn, to_half] = spectra[:, to_half * 2 * width : (to_half + 1) * 2 * width]
        copy = pltpu.make_async_remote_copy(
            src_ref=opt_send.at[turn, other_half],
            dst_ref=opt_cols.at[turn, rows],
            send_sem=opt_ssem.at[turn],
            recv_sem=opt_rsem.at[turn],
            device_id={"half": other_half},
            device_id_type=MESH,
        )
        copy.start()
        opt_copies.append(copy)
        opt_cols[turn, rows, :] = opt_send[turn, half]

    slot_of = []
    for run in range(halves):
        places = []
        for source in range(group):
            place = jnp.int32(0)
            for j in range(group):
                spot = dest_ref[source * group + j]
                place = jnp.where(
                    lax.div(spot, group) == tile * halves + run, lax.rem(spot, group), place
                )
            places.append(place)
        for slot in range(group):
            found = jnp.int32(0)
            for source in range(group):
                found = jnp.where(places[source] == slot, source, found)
            slot_of.append(found)

    for step in order:
        for shift in range(halves):
            if step or shift:
                source = lax.rem(tile + step, tiles) * halves + lax.rem(half + shift, halves)
                pltpu.make_async_remote_copy(
                    src_ref=sar_send.at[0, 0],
                    dst_ref=arrived.at[source],
                    send_sem=sar_ssem.at[0],
                    recv_sem=sar_rsem.at[source],
                    device_id={"half": other_half},
                    device_id_type=MESH,
                ).wait_recv()
    per_patch = group // patch_dev
    for run in range(halves):
        for slot in range(group):
            at = run * quarter + (slot % per_patch) * lines
            sar_cols[slot // per_patch, at : at + lines, :] = arrived[slot_of[run * group + slot], run]

    loads[3].wait()
    for patch in range(patch_dev):
        for c in range(chunks):
            sar_rows[patch, c] = jnp.dot(
                row_v[c], sar_cols[patch], preferred_element_type=jnp.float32
            )

    lane = lax.broadcasted_iota(jnp.int32, (chunk, width), 1)
    line = lax.broadcasted_iota(jnp.int32, (chunk, width), 0)
    shared = (lane + half) == 0
    centre = (lane + line + half) == 0

    def parts(table_rows, first):
        a, c = table_rows[:chunk, :width], table_rows[:chunk, width:]
        b, d = table_rows[chunk:, :width], table_rows[chunk:, width:]
        if first:
            a = jnp.where(centre, 0.0, a)
        return a, b, c, d

    def cross_chunk(turn, patch, c):
        oa, ob, oc, od = parts(
            jnp.dot(row_v[c], opt_cols[turn], preferred_element_type=jnp.float32), c == 0
        )
        sa, sb, sc, sd = parts(sar_rows[patch, c], c == 0)
        o_re, o_im, s_re, s_im = oa + od, oc - ob, sa + sd, sc - sb
        real = o_re * s_re + o_im * s_im
        imag = o_re * s_im - o_im * s_re
        shared_real = oa * sa + ob * sb - (od * sc - oc * sd)
        shared_imag = ob * sa - oa * sb + (oc * sc + od * sd)
        real = jnp.where(shared, shared_real, real)
        imag = jnp.where(shared, shared_imag, imag)
        o_energy = jnp.sum(o_re * o_re + o_im * o_im, axis=0, keepdims=True)
        s_energy = jnp.sum(s_re * s_re + s_im * s_im, axis=0, keepdims=True)
        return real, imag, o_energy, s_energy

    weight = jnp.where(shared[:1], 1.0, 2.0)

    def pair_copy(k, src, dst, axis, to):
        return pltpu.make_async_remote_copy(
            src_ref=src,
            dst_ref=dst,
            send_sem=pair_ssem.at[k],
            recv_sem=pair_rsem.at[k],
            device_id={axis: to},
            device_id_type=MESH,
        )

    opt_copies[0].wait_recv()
    o_sum, s_sum = 0.0, 0.0
    for c in range(chunks):
        real, imag, o_energy, s_energy = cross_chunk(0, other_band, c)
        cross_send[c, :, :width] = real.astype(jnp.bfloat16)
        cross_send[c, :, width:] = imag.astype(jnp.bfloat16)
        o_sum, s_sum = o_sum + o_energy, s_sum + s_energy
    stat_send[0:1, :] = o_sum * weight
    stat_send[1:2, :] = s_sum * weight
    stat_send[2:8, :] = jnp.zeros((6, width), jnp.float32)
    cross_copy = pair_copy(0, cross_send, cross_recv, "band", other_band)
    cross_copy.start()
    stat_copy = pair_copy(1, stat_send, stat_recv, "band", other_band)
    stat_copy.start()

    cross_copy.wait_recv()
    opt_copies[1].wait_recv()
    o_sum, s_sum = 0.0, 0.0
    for c in range(chunks):
        real, imag, o_energy, s_energy = cross_chunk(1, band, c)
        at = slice(c * chunk, (c + 1) * chunk)
        real = real + cross_recv[c, :, :width].astype(jnp.float32)
        imag = imag + cross_recv[c, :, width:].astype(jnp.float32)
        cross_all[at, :width] = real.astype(jnp.bfloat16)
        cross_all[at, width:] = imag.astype(jnp.bfloat16)
        o_sum, s_sum = o_sum + o_energy, s_sum + s_energy

    loads[4].wait()

    def lag_chunk(c):
        both = jnp.dot(row_v[c], cross_all[...], preferred_element_type=jnp.float32)
        lags[c, :, :width] = (both[:chunk, :width] - both[chunk:, width:]).astype(jnp.bfloat16)
        lags[c, :, width:] = (both[:chunk, width:] + both[chunk:, :width]).astype(jnp.bfloat16)

    lag_copies = []
    for i in range(per_half):
        at = other_half * per_half + i
        lag_chunk(at)
        copy = pair_copy(3 + i, lags.at[at], lag_recv.at[i], "half", other_half)
        copy.start()
        lag_copies.append(copy)
    for i in range(per_half):
        lag_chunk(half * per_half + i)

    spots = lax.broadcasted_iota(jnp.int32, (peak_count, extent), 1)
    ranks = lax.broadcasted_iota(jnp.int32, (peak_count, extent), 0)

    loads[6].wait()

    def one_hot(which):
        wanted = jnp.zeros((peak_count, extent), jnp.int32)
        for j in range(peak_count):
            wanted = jnp.where(ranks == j, peaks_ref[0, which, j], wanted)
        return jnp.where(spots == wanted, 1.0, 0.0).astype(jnp.bfloat16)

    picked = jnp.dot(
        one_hot(0), lags[...].reshape(extent, 2 * width), preferred_element_type=jnp.float32
    )
    waves = lax.dot_general(
        one_hot(1), lag_v[half], (((1,), (1,)), ((), ())), preferred_element_type=jnp.float32
    )
    stat_copy.wait_recv()
    last_send[0:8, :] = stat_recv[...]
    last_send[0:1, :] = o_sum * weight + stat_recv[0:1, :]
    last_send[1:2, :] = s_sum * weight + stat_recv[1:2, :]
    last_send[8 : 8 + peak_count, :] = jnp.broadcast_to(
        jnp.sum(picked * waves, axis=1, keepdims=True), (peak_count, width)
    )
    last_copy = pair_copy(2, last_send, last_recv, "half", other_half)
    last_copy.start()

    for i in range(per_half):
        at = slice(i * chunk, (i + 1) * chunk)
        near = lags[half * per_half + i]
        surface_ref[0, at, :] = jnp.dot(near, lag_v[half], preferred_element_type=jnp.float32)

    for i in range(per_half):
        at = slice(i * chunk, (i + 1) * chunk)
        lag_copies[i].wait_recv()
        far = jnp.dot(lag_recv[i], lag_v[other_half], preferred_element_type=jnp.float32)
        surface_ref[0, at, :] = surface_ref[0, at, :] + far

    last_copy.wait_recv()
    total_ref[...] = last_send[...] + last_recv[...]
    for copy in copies + opt_copies + lag_copies + [cross_copy, stat_copy, last_copy]:
        copy.wait_send()


def finish(bands, pieces, surface_ref, total_ref, out_ref, peak_ref, scaled, sem):
    _, lines, extent = surface_ref.shape
    pixels = extent * extent
    peak_count = peak_ref.shape[1]
    width = total_ref.shape[1]
    o_all = jnp.sum(total_ref[0:1, :], axis=1, keepdims=True) / (float(pixels) * bands * pixels)
    s_all = jnp.sum(total_ref[1:2, :], axis=1, keepdims=True) / (float(pixels) * bands * pixels)
    norm = lax.rsqrt(bands * pixels * (o_all + EPSILON) * (s_all + EPSILON)) / pixels
    part = lines // pieces
    copies = []
    for i in range(pieces):
        at = pl.ds(i * part, part)
        scaled[at, :] = surface_ref[0, at, :] * norm
        copy = pltpu.make_async_copy(scaled.at[at], out_ref.at[0, at], sem.at[i])
        copy.start()
        copies.append(copy)
    values = total_ref[8 : 8 + peak_count, :] * norm
    lane = lax.broadcasted_iota(jnp.int32, (peak_count, width), 1)
    rank = lax.broadcasted_iota(jnp.int32, (peak_count, width), 0)
    row = jnp.sum(jnp.where(lane == rank, values, 0.0), axis=0, keepdims=True)
    peak_ref[...] = row[:, :peak_count]
    for copy in copies:
        copy.wait()


def fused(mesh, optical, sar, destination, peaks):
    tiles, halves, bands = mesh.shape["tile"], mesh.shape["half"], mesh.shape["band"]
    patch_dev, _, quarter, extent = optical.shape
    group = tiles * halves
    lines = sar.shape[1] // group
    peak_count = peaks.shape[2]
    chunk = quarter // 2
    chunks = extent // chunk
    width = extent // 2 // halves
    sizes = (tiles, halves, bands, patch_dev, quarter, extent, lines, chunk, peak_count)
    tables = half_tables(extent, halves, chunk)
    bf, f32 = jnp.bfloat16, jnp.float32
    wide = 2 * width
    vmem = pltpu.VMEM
    dma = pltpu.SemaphoreType.DMA
    raw, totals = pl.pallas_call(
        functools.partial(kernel, sizes),
        out_shape=(
            jax.ShapeDtypeStruct((1, quarter, extent), f32),
            jax.ShapeDtypeStruct((8 + peak_count, width), f32),
        ),
        in_specs=[pl.BlockSpec(memory_space=pltpu.HBM)] * 7,
        out_specs=(pl.BlockSpec(memory_space=pltpu.VMEM), pl.BlockSpec(memory_space=pltpu.VMEM)),
        scratch_shapes=[
            pltpu.SMEM(destination.shape, jnp.int32),
            pltpu.SMEM(peaks.shape, jnp.int32),
            vmem((group, lines, extent), bf),
            vmem((patch_dev, quarter, extent), bf),
            vmem((extent, extent), bf),
            vmem((chunks, 2 * chunk, extent), bf),
            vmem((halves, wide, extent), bf),
            vmem((tiles, halves, halves, lines, wide), bf),
            vmem((group, halves, lines, wide), bf),
            vmem((patch_dev, halves, quarter, wide), bf),
            vmem((patch_dev, extent, wide), bf),
            vmem((patch_dev, extent, wide), bf),
            vmem((patch_dev, chunks, 2 * chunk, wide), f32),
            vmem((chunks, chunk, wide), bf),
            vmem((chunks, chunk, wide), bf),
            vmem((extent, wide), bf),
            vmem((8, width), f32),
            vmem((8, width), f32),
            vmem((8 + peak_count, width), f32),
            vmem((8 + peak_count, width), f32),
            vmem((chunks, chunk, wide), bf),
            vmem((chunks // halves, chunk, wide), bf),
            dma((7,)),
            dma((group,)),
            dma((group,)),
            dma((2,)),
            dma((2,)),
            dma((3 + chunks // halves,)),
            dma((3 + chunks // halves,)),
        ],
        compiler_params=pltpu.CompilerParams(
            collective_id=0, has_side_effects=True, vmem_limit_bytes=50 * 1024 * 1024
        ),
    )(
        *[
            pltpu.with_memory_space_constraint(x, pltpu.HBM)
            for x in (
                destination,
                peaks,
                sar.reshape(group, lines, extent),
                optical.reshape(patch_dev, quarter, extent),
                *[jnp.asarray(t) for t in tables],
            )
        ]
    )
    pieces = 2
    return pl.pallas_call(
        functools.partial(finish, bands, pieces),
        out_shape=(
            jax.ShapeDtypeStruct((1, quarter, extent), f32),
            jax.ShapeDtypeStruct((1, peak_count), f32),
        ),
        in_specs=[pl.BlockSpec(memory_space=pltpu.VMEM)] * 2,
        out_specs=(pl.BlockSpec(memory_space=pltpu.HBM), pl.BlockSpec(memory_space=pltpu.VMEM)),
        scratch_shapes=[vmem((quarter, extent), f32), dma((pieces,))],
    )(*[pltpu.with_memory_space_constraint(x, pltpu.VMEM) for x in (raw, totals)])


def fits(mesh, optical, sar, peaks):
    group = mesh.shape["tile"] * mesh.shape["half"]
    patch_dev, local_bands, quarter, extent = optical.shape
    lines = sar.shape[1] // group
    return (
        mesh.shape["half"] == 2
        and mesh.shape["band"] == 2
        and patch_dev == 2
        and local_bands == 1
        and lines % 16 == 0
        and quarter % lines == 0
        and extent % 512 == 0
        and peaks.shape[0] == 1
        and peaks.shape[2] % 8 == 0
    )


def solution(mesh):
    def local(optical, sar, destination, peaks):
        if fits(mesh, optical, sar, peaks):
            return fused(mesh, optical, sar, destination, peaks)
        return generic(optical, sar, destination, peaks)

    in_specs = (
        P(("scene", "tile"), "band", "half", None),
        P("band", ("scene", "tile", "half"), None),
        P("scene"),
        P(("scene", "tile", "band"), None, None),
    )
    out_specs = (P(("scene", "tile", "band"), "half", None), P(("scene", "tile", "band"), None))
    return jax.shard_map(local, mesh=mesh, in_specs=in_specs, out_specs=out_specs, check_vma=False)
```
